32 devices in a mesh: chan: 4 (over x, core), slab: 8 (over z, y).
Axes of the slice: x: 2, y: 2, z: 4, core: 2. Of those that a mesh axis runs over, the one named last changes fastest.
Arguments:
- beam_images: float32 [64, 512, 4096], P('chan', 'slab'), may hold values from -24 to 24
- chan_weights: int32 [64], P('chan'), may hold values from 1 to 8
- freq_offsets: float32 [64], P('chan'), may hold values from -1 to 1
- half_widths: int32 [5], replicated, may hold values from 16 to 32, as said below
Outputs:
- smoothed: float32 [5, 512, 4096], P(None, 'slab', 'chan')
The draws below stay inside these ranges and needn't reach their ends.
Inputs may be any that keep to these rules, and one draw needn't show every extreme that they name: `half_widths`: each half-width is at least 16 and at most 32; at least one equals 32.
All inputs are finite; a program needn't handle non-finite values.
Results may differ from the reference program's by a relative error of at most 0.00008.
Values sent between devices are 32-bit elements; how exact they have to be, the bound alone decides.
A program may use at most 128 MiB of HBM per device.

```python
import jax
import jax.numpy as jnp
from jax import lax

NCHAN = 64
NCOLS = 4096
MOMENTS = 5
HW_MAX = 32
NROWS = 512


def draw_half_widths(key, part):
    first_key, second_key = jax.random.split(jax.random.fold_in(key, 17))
    values = jax.random.randint(first_key, (MOMENTS,), HW_MAX // 2, HW_MAX + 1)
    chosen = jax.random.randint(second_key, (), 0, MOMENTS)
    return jnp.where(jnp.arange(MOMENTS) == chosen, HW_MAX, values).astype(jnp.int32)


def with_ends(array, stream_key, low, largest):
    dims = array.shape
    spot = [jax.random.randint(jax.random.fold_in(stream_key, axis), (), 0, dims[axis]) for axis in range(len(dims))]
    array = array.at[tuple(spot)].set(low)
    longest = dims.index(max(dims))
    spot[longest] = (spot[longest] + 1) % dims[longest]
    return array.at[tuple(spot)].set(largest)


def block_scale(stream_key, extent, cuts, smallest, largest):
    gain, own = 1.0, jax.random.fold_in(stream_key, 6)
    for axis_at, blocks in cuts:
        heights = jnp.exp(jax.random.uniform(jax.random.fold_in(own, axis_at), (blocks,), jnp.float32, smallest / len(cuts), largest / len(cuts)))
        gain = gain * jnp.repeat(heights, extent[axis_at] // blocks).reshape([-1 if axis == axis_at else 1 for axis in range(len(extent))])
    return gain


def gaussian(own_key, extent, deviation, bound, pieces=(), dtype=jnp.bfloat16):
    result = jax.random.normal(own_key, extent, jnp.float32) * deviation
    if len(pieces) > 0:
        result = block_scale(own_key, extent, pieces, -0.22, 0.18) * result
    return jnp.clip(result, min=-bound, max=bound).astype(dtype)


def setup_inputs(seed: int = 0) -> dict:
    streams_of = jax.random.split(jax.random.key(seed), 5)
    return {
        "beam_images": gaussian(streams_of[0], (NCHAN, NROWS, NCOLS), 4.0, 24.0, ((0, 4), (1, 8)), jnp.float32),
        "chan_weights": with_ends(jax.random.randint(streams_of[1], (NCHAN,), 1, 9), jax.random.fold_in(streams_of[1], 1), 1, 8).astype(jnp.int32),
        "freq_offsets": jnp.clip(jax.random.uniform(streams_of[2], (NCHAN,), jnp.float32, -1.0, 1.0) * block_scale(streams_of[2], (NCHAN,), ((0, 4),), -0.4, 0.0), -1.0, 1.0),
        "half_widths": draw_half_widths(jax.random.fold_in(streams_of[4], 71), 0),
    }


def window_sum(values, reach, along):
    length = values.shape[along]
    widths = [(0, 0)] * values.ndim
    widths[along] = (HW_MAX + 1, HW_MAX)
    padded = jnp.pad(values, widths)
    running = jnp.cumsum(padded, axis=along)
    upper = lax.dynamic_slice_in_dim(running, (HW_MAX + 1 + reach).astype(jnp.int32), length, along)
    lower = lax.dynamic_slice_in_dim(running, (HW_MAX - reach).astype(jnp.int32), length, along)
    return upper - lower


def reference(beam_images, chan_weights, freq_offsets, half_widths):
    weight_floats = chan_weights.astype(jnp.float32)
    weight_total = jnp.sum(weight_floats)
    powers = jnp.stack([freq_offsets ** power for power in range(MOMENTS)])
    coefficients = powers * weight_floats[None, :] / weight_total
    flat = beam_images.reshape(NCHAN, NROWS * NCOLS)
    moments = jnp.dot(coefficients, flat, precision=lax.Precision.HIGHEST, preferred_element_type=jnp.float32)
    moments = moments.reshape(MOMENTS, NROWS, NCOLS)
    results = []
    for power in range(MOMENTS):
        reach = half_widths[power]
        summed = window_sum(window_sum(moments[power], reach, 0), reach, 1)
        results.append(summed / (2 * reach + 1).astype(jnp.float32))
    return jnp.stack(results)
```

```python
import functools

import jax
import jax.numpy as jnp
from jax import lax
from jax.experimental import pallas as pl
from jax.experimental.pallas import tpu as pltpu
from jax.sharding import PartitionSpec as P

MOMENTS = 5
HW_MAX = 32
LANES = 128
HALF = LANES // 2
PARTS = 2
ROWS_AT_ONCE = 32
MESH = pl.DeviceIdType.MESH


def split(value):
    parts = []
    for _ in range(PARTS - 1):
        part = value.astype(jnp.bfloat16)
        parts.append(part)
        value = value - part.astype(jnp.float32)
    parts.append(value.astype(jnp.bfloat16))
    return parts


def kernel(
    chans, slabs,
    w_hbm, f_hbm, h_hbm, beam_ref, out_ref,
    w_ref, f_ref, h_ref,
    beams, pieces, band, row_band, sums, passed, crossed, ext, weights, scale,
    small_sem, load_sem, first_send, first_recv, pass_send, pass_recv, cross_send, cross_recv,
    up_send, up_recv, down_send, down_recv, w_send, w_recv,
):
    groups = chans // 2
    me = lax.axis_index("chan")
    slab = lax.axis_index("slab")
    group, core = me // 2, lax.rem(me, 2)
    local_chans, rows, all_cols = beam_ref.shape
    width = all_cols // chans
    chunks = width // LANES
    edge = chunks - 1
    own = groups - 1
    partner = group * 2 + (1 - core)
    not_first, not_last = slab > 0, slab < slabs - 1

    def block_of(slot):
        owner_group = lax.rem(group + slot // 2 + 1, groups)
        return owner_group * 2 + (1 - core if slot % 2 == 0 else core)

    def load(slot, tile):
        col = pl.multiple_of((block_of(slot) * chunks + tile) * LANES, LANES)
        return pltpu.make_async_copy(
            beam_ref.at[:, :, pl.ds(col, LANES)], beams.at[slot, tile], load_sem.at[slot, tile]
        )

    small = [
        pltpu.make_async_copy(source, target, small_sem.at[at])
        for at, (source, target) in enumerate(((h_hbm, h_ref), (w_hbm, w_ref), (f_hbm, f_ref)))
    ]
    for copy in small:
        copy.start()
    for slot in range(chans):
        for tile in range(2):
            load(slot, tile).start()

    @pl.loop(2, chunks)
    def _(tile):
        for slot in range(chans):
            load(slot, tile).start()

    barrier = pltpu.get_barrier_semaphore()
    for offset in range(1, chans):
        pl.semaphore_signal(
            barrier, inc=1, device_id={"chan": lax.rem(me + offset, chans)}, device_id_type=MESH
        )

    @pl.when(not_first)
    def _():
        pl.semaphore_signal(barrier, inc=1, device_id={"slab": slab - 1}, device_id_type=MESH)

    @pl.when(not_last)
    def _():
        pl.semaphore_signal(barrier, inc=1, device_id={"slab": slab + 1}, device_id_type=MESH)

    source = lax.broadcasted_iota(jnp.int32, (2 * LANES, LANES), 0)
    lane = lax.broadcasted_iota(jnp.int32, (2 * LANES, LANES), 1)
    for copy in small:
        copy.wait()

    def put_band(kind, k, near):
        band[kind, k] = jnp.where(near, 1.0, 0.0).astype(jnp.bfloat16)

    target = jnp.where(lane < HALF, lane + LANES, lane)

    @pl.loop(0, MOMENTS)
    def _(k):
        put_band(0, k, jnp.abs(source - target) <= h_ref[k])

    def weight_copy(offset):
        return pltpu.make_async_remote_copy(
            src_ref=weights.at[0], dst_ref=weights.at[offset],
            send_sem=w_send.at[offset - 1], recv_sem=w_recv.at[offset - 1],
            device_id={"chan": lax.rem(me + offset, chans)}, device_id_type=MESH,
        )

    def pass_copy(hop, c):
        return pltpu.make_async_remote_copy(
            src_ref=sums.at[2 * hop, c], dst_ref=passed.at[hop, c],
            send_sem=pass_send.at[hop, c], recv_sem=pass_recv.at[hop, c],
            device_id={"chan": partner}, device_id_type=MESH,
        )

    def first_copy(k):
        return pltpu.make_async_remote_copy(
            src_ref=sums.at[0, 0, k], dst_ref=passed.at[0, 0, k],
            send_sem=first_send.at[k], recv_sem=first_recv.at[k],
            device_id={"chan": partner}, device_id_type=MESH,
        )

    def cross_copy(hop, c, k):
        other = lax.rem(group + hop + 1, groups) * 2 + core
        return pltpu.make_async_remote_copy(
            src_ref=sums.at[2 * hop + 1, c, k], dst_ref=crossed.at[hop, c, k],
            send_sem=cross_send.at[hop, c, k], recv_sem=cross_recv.at[hop, c, k],
            device_id={"chan": other}, device_id_type=MESH,
        )

    def up_copy(c, k):
        return pltpu.make_async_remote_copy(
            src_ref=ext.at[c, k, pl.ds(HW_MAX, HW_MAX)],
            dst_ref=ext.at[c, k, pl.ds(HW_MAX + rows, HW_MAX)],
            send_sem=up_send.at[c, k], recv_sem=up_recv.at[c, k],
            device_id={"slab": slab - 1}, device_id_type=MESH,
        )

    def down_copy(c, k):
        return pltpu.make_async_remote_copy(
            src_ref=ext.at[c, k, pl.ds(rows, HW_MAX)],
            dst_ref=ext.at[c, k, pl.ds(0, HW_MAX)],
            send_sem=down_send.at[c, k], recv_sem=down_recv.at[c, k],
            device_id={"slab": slab + 1}, device_id_type=MESH,
        )

    def moments_of(slot, tile):
        load(slot, tile).wait()
        cols = pl.ds(pl.multiple_of((block_of(slot) * chunks + tile + 1) * LANES, LANES), LANES)

        @pl.loop(0, rows // ROWS_AT_ONCE)
        def _(part):
            first = pl.multiple_of(part * ROWS_AT_ONCE, ROWS_AT_ONCE)
            totals = [None] * MOMENTS
            for chan in range(local_chans):
                weight = w_ref[chan].astype(jnp.float32)
                offset = f_ref[chan]
                term = beams[slot, tile, chan, pl.ds(first, ROWS_AT_ONCE), :] * weight
                for k in range(MOMENTS):
                    if k > 0:
                        term = term * offset
                    totals[k] = term if chan == 0 else totals[k] + term
            for k in range(MOMENTS):
                for at, piece in enumerate(split(totals[k])):
                    pieces[k, pl.ds(first + at * rows, ROWS_AT_ONCE), cols] = piece

    def fold(product):
        result = product[:rows]
        for at in range(1, PARTS):
            result = result + product[at * rows : (at + 1) * rows]
        return result

    def lanes_from(slot, tile):
        first = (block_of(slot) * chunks + tile + 1) * LANES
        return pl.ds(pl.multiple_of(first, LANES), 2 * LANES)

    def columns_of(slot, c, after=None):
        wide = lanes_from(slot, c)
        for k in range(MOMENTS):
            sums[slot, c, k] = fold(
                jnp.dot(pieces[k, :, wide], band[0, k], preferred_element_type=jnp.float32)
            )
            if after is not None:
                after(k)

    def edge_of(slot):
        low, high = lanes_from(slot, -1), lanes_from(slot, chunks - 1)
        for k in range(MOMENTS):
            sums[slot, edge, k] = fold(
                jnp.dot(pieces[k, :, low], band[1, k], preferred_element_type=jnp.float32)
                + jnp.dot(pieces[k, :, high], band[2, k], preferred_element_type=jnp.float32)
            )

    def make(slot, c):
        if isinstance(c, int) and c == edge:
            edge_of(slot)
        else:
            moments_of(slot, c + 1)
            columns_of(slot, c)
        if slot % 2 == 0:
            pass_copy(slot // 2, c).start()

    def send_on(hop, c):
        pass_copy(hop, c).wait_recv()
        for k in range(MOMENTS):
            sums[2 * hop + 1, c, k] = sums[2 * hop + 1, c, k] + passed[hop, c, k]
            cross_copy(hop, c, k).start()

    def finish(c, k):
        value = sums[chans - 1, c, k] + passed[own, c, k]
        for hop in range(own):
            cross_copy(hop, c, k).wait_recv()
            value = value + crossed[hop, c, k]
        ext[c, k, HW_MAX : HW_MAX + rows, :] = value

        @pl.when(not_first)
        def _():
            up_copy(c, k).start()

        @pl.when(not_last)
        def _():
            down_copy(c, k).start()

    left = lax.broadcasted_iota(jnp.int32, (rows, LANES), 1) < HALF

    def rows_of(c, k):
        @pl.when(not_last)
        def _():
            up_copy(c, k).wait_recv()

        @pl.when(not_first)
        def _():
            down_copy(c, k).wait_recv()

        both = jnp.concatenate(split(ext[c, k]), axis=0)
        summed = jnp.dot(row_band[k], both, preferred_element_type=jnp.float32)
        summed = summed * scale[k, 0:1, :]
        if isinstance(c, int) and c == edge:
            at, to = slice(0, LANES), slice(edge * LANES, chunks * LANES)
            out_ref[k, :, at] = jnp.where(left, summed, out_ref[k, :, at])
            out_ref[k, :, to] = jnp.where(left, out_ref[k, :, to], summed)
        else:
            at = pl.ds(pl.multiple_of(c * LANES, LANES), LANES)
            to = pl.ds(pl.multiple_of((c + 1) * LANES, LANES), LANES)
            if isinstance(c, int) and c == 0:
                out_ref[k, :, at] = summed
            else:
                out_ref[k, :, at] = jnp.where(left, out_ref[k, :, at], summed)
            out_ref[k, :, to] = summed

    for slot in range(2):
        moments_of(slot, 0)
        moments_of(slot, 1)
        if slot == 0:
            pl.semaphore_wait(
                barrier, chans - 1 + not_first.astype(jnp.int32) + not_last.astype(jnp.int32)
            )
            columns_of(slot, 0, lambda k: first_copy(k).start())
        else:
            columns_of(slot, 0)
    for k in range(MOMENTS):
        first_copy(k).wait_recv()
        sums[1, 0, k] = sums[1, 0, k] + passed[0, 0, k]
        if own > 0:
            cross_copy(0, 0, k).start()

    total = w_ref[0].astype(jnp.float32)
    for chan in range(1, local_chans):
        total = total + w_ref[chan].astype(jnp.float32)
    weights[0] = jnp.full(weights.shape[1:], total, jnp.float32)
    for offset in range(1, chans):
        weight_copy(offset).start()

    for slot in range(2, chans):
        moments_of(slot, 0)
        make(slot, 0)
    for hop in range(1, own):
        send_on(hop, 0)
    for slot in range(chans):
        make(slot, 1)
    for hop in range(own):
        send_on(hop, 1)
    pass_copy(own, 0).wait_recv()

    @pl.when(slab == 0)
    def _():
        @pl.loop(0, chunks)
        def _(c):
            ext[c, :, 0:HW_MAX, :] = jnp.zeros((MOMENTS, HW_MAX, LANES), jnp.float32)

    @pl.when(slab == slabs - 1)
    def _():
        @pl.loop(0, chunks)
        def _(c):
            ext[c, :, HW_MAX + rows :, :] = jnp.zeros((MOMENTS, HW_MAX, LANES), jnp.float32)

    def set_rest():
        pieces[:, :, 0:LANES] = jnp.zeros(pieces.shape[:2] + (LANES,), jnp.bfloat16)
        pieces[:, :, LANES + all_cols :] = jnp.zeros(pieces.shape[:2] + (LANES,), jnp.bfloat16)
        for offset in range(1, chans):
            weight_copy(offset).wait_recv()
        weight_total = weights[0]
        for offset in range(1, chans):
            weight_total = weight_total + weights[offset]

        @pl.loop(0, MOMENTS)
        def _(k):
            reach = h_ref[k]
            near = jnp.logical_and(lane < HALF, jnp.abs(source - LANES - lane) <= reach)
            put_band(1, k, near)
            near = jnp.logical_and(lane >= HALF, jnp.abs(source - lane) <= reach)
            put_band(2, k, near)
            span = rows + 2 * HW_MAX
            to_row = lax.broadcasted_iota(jnp.int32, (rows, span), 0)
            from_row = lax.broadcasted_iota(jnp.int32, (rows, span), 1)
            near = jnp.abs(from_row - HW_MAX - to_row) <= reach
            near = jnp.where(near, 1.0, 0.0).astype(jnp.bfloat16)
            for part in range(PARTS):
                row_band[k, :, part * span : (part + 1) * span] = near
            divisor = weight_total * (2 * reach + 1).astype(jnp.float32)
            scale[k] = 1.0 / divisor

    def iteration(c, ahead, behind):
        jobs = []
        if ahead is not None:
            for hop in range(own):
                jobs += [functools.partial(make, 2 * hop, ahead)]
                jobs += [functools.partial(make, 2 * hop + 1, ahead)]
            jobs += [functools.partial(make, 2 * own, ahead)]

            def last():
                for hop in range(own):
                    send_on(hop, ahead)
                make(chans - 1, ahead)

            jobs.append(last)
        for k in range(MOMENTS):
            finish(c, k)
            if k < MOMENTS - 1:
                share = -(-len(jobs) // (MOMENTS - 1 - k))
                for job in jobs[:share]:
                    job()
                jobs = jobs[share:]
            if behind is not None:
                rows_of(behind, k)
        if not (isinstance(c, int) and c == edge):
            pass_copy(own, c + 1).wait_recv()

    iteration(0, 2, None)
    set_rest()
    iteration(1, 3, None)
    iteration(2, 4, 0)

    @pl.loop(3, edge - 2)
    def _(c):
        iteration(c, c + 2, c - 2)

    iteration(edge - 2, edge, edge - 4)
    iteration(edge - 1, None, edge - 3)
    iteration(edge, None, edge - 2)

    for k in range(MOMENTS):
        rows_of(edge - 1, k)

    def sent(c):
        for hop in range(groups):
            if not (isinstance(c, int) and c == 0 and hop == 0):
                pass_copy(hop, c).wait_send()
        for k in range(MOMENTS):
            for hop in range(own):
                cross_copy(hop, c, k).wait_send()

            @pl.when(not_first)
            def _():
                up_copy(c, k).wait_send()

            @pl.when(not_last)
            def _():
                down_copy(c, k).wait_send()

    for offset in range(1, chans):
        weight_copy(offset).wait_send()
    for k in range(MOMENTS):
        first_copy(k).wait_send()
    sent(0)

    @pl.loop(1, chunks - 1)
    def _(c):
        sent(c)

    for k in range(MOMENTS):
        rows_of(edge, k)
    sent(edge)


def body(chans, slabs, beam_images, chan_weights, freq_offsets, half_widths):
    local_chans, rows, all_cols = beam_images.shape
    width = all_cols // chans
    chunks, groups = width // LANES, chans // 2
    f32, b16 = jnp.float32, jnp.bfloat16
    dma = pltpu.SemaphoreType.DMA
    hbm = pl.BlockSpec(memory_space=pltpu.HBM)
    small = [
        pltpu.with_memory_space_constraint(value, pltpu.HBM)
        for value in (chan_weights, freq_offsets, half_widths)
    ]
    span = rows + 2 * HW_MAX
    return pl.pallas_call(
        functools.partial(kernel, chans, slabs),
        out_shape=jax.ShapeDtypeStruct((MOMENTS, rows, width), f32),
        in_specs=[hbm, hbm, hbm, hbm],
        out_specs=pl.BlockSpec(memory_space=pltpu.VMEM),
        scratch_shapes=[
            pltpu.SMEM(chan_weights.shape, jnp.int32),
            pltpu.SMEM(freq_offsets.shape, f32),
            pltpu.SMEM(half_widths.shape, jnp.int32),
            pltpu.VMEM((chans, chunks, local_chans, rows, LANES), f32),
            pltpu.VMEM((MOMENTS, PARTS * rows, all_cols + 2 * LANES), b16),
            pltpu.VMEM((3, MOMENTS, 2 * LANES, LANES), b16),
            pltpu.VMEM((MOMENTS, rows, PARTS * span), b16),
            pltpu.VMEM((chans, chunks, MOMENTS, rows, LANES), f32),
            pltpu.VMEM((groups, chunks, MOMENTS, rows, LANES), f32),
            pltpu.VMEM((groups - 1, chunks, MOMENTS, rows, LANES), f32),
            pltpu.VMEM((chunks, MOMENTS, span, LANES), f32),
            pltpu.VMEM((chans, 8, LANES), f32),
            pltpu.VMEM((MOMENTS, 8, LANES), f32),
            dma((3,)),
            dma((chans, chunks)),
            dma((MOMENTS,)),
            dma((MOMENTS,)),
            dma((groups, chunks)),
            dma((groups, chunks)),
            dma((groups - 1, chunks, MOMENTS)),
            dma((groups - 1, chunks, MOMENTS)),
            dma((chunks, MOMENTS)),
            dma((chunks, MOMENTS)),
            dma((chunks, MOMENTS)),
            dma((chunks, MOMENTS)),
            dma((chans - 1,)),
            dma((chans - 1,)),
        ],
        compiler_params=pltpu.CompilerParams(
            collective_id=0, has_side_effects=True, vmem_limit_bytes=44 * 1024 * 1024
        ),
    )(*small, beam_images)


def solution(mesh):
    placed = (P("chan", "slab", None), P("chan"), P("chan"), P())
    return jax.shard_map(
        functools.partial(body, mesh.shape["chan"], mesh.shape["slab"]),
        mesh=mesh, in_specs=placed, out_specs=P(None, "slab", "chan"), check_vma=False,
    )
```

```python
import functools

import jax
import jax.numpy as jnp
from jax import lax
from jax.experimental import pallas as pl
from jax.experimental.pallas import tpu as pltpu
from jax.sharding import PartitionSpec as P

MOMENTS = 5
HW_MAX = 32
LANES = 128
HALF = LANES // 2
PARTS = 2
ROWS_AT_ONCE = 32
FIRST = 2
PASS_TURNS = 3
CROSS_TURNS = 4
ROW_TURNS = 5
MESH = pl.DeviceIdType.MESH


def split(value):
    parts = []
    for _ in range(PARTS - 1):
        part = value.astype(jnp.bfloat16)
        parts.append(part)
        value = value - part.astype(jnp.float32)
    parts.append(value.astype(jnp.bfloat16))
    return parts


def kernel(
    chans, slabs,
    w_hbm, f_hbm, h_hbm, beam_ref, out_ref,
    w_ref, f_ref, h_ref,
    beams, pieces, band, row_band, sums, passed, crossed, ext, weights, scale,
    small_sem, first_sem, load_sem, pass_send, pass_recv, cross_send, cross_recv,
    up_send, up_recv, down_send, down_recv, w_send, w_recv,
):
    groups = chans // 2
    me = lax.axis_index("chan")
    slab = lax.axis_index("slab")
    group, core = me // 2, lax.rem(me, 2)
    local_chans, rows, all_cols = beam_ref.shape
    width = all_cols // chans
    chunks = width // LANES
    edge = chunks - 1
    own = groups - 1
    partner = group * 2 + (1 - core)
    not_first, not_last = slab > 0, slab < slabs - 1

    def block_of(slot):
        owner_group = lax.rem(group + slot // 2 + 1, groups)
        return owner_group * 2 + (1 - core if slot % 2 == 0 else core)

    def load(slot, tile):
        col = pl.multiple_of((block_of(slot) * chunks + tile) * LANES, LANES)
        sem = first_sem.at[slot] if isinstance(tile, int) else load_sem.at[tile - FIRST]
        return pltpu.make_async_copy(
            beam_ref.at[:, :, pl.ds(col, LANES)], beams.at[tile, slot], sem
        )

    def drain(ref, sem):
        pltpu.make_async_copy(ref, ref, sem).wait()

    small = [
        pltpu.make_async_copy(source, target, small_sem.at[at])
        for at, (source, target) in enumerate(((h_hbm, h_ref), (w_hbm, w_ref), (f_hbm, f_ref)))
    ]
    for copy in small:
        copy.start()
    for slot in range(chans):
        for tile in range(FIRST):
            load(slot, tile).start()

    @pl.loop(FIRST, chunks)
    def _(tile):
        for slot in range(chans):
            load(slot, tile).start()

    barrier = pltpu.get_barrier_semaphore()
    for offset in range(1, chans):
        pl.semaphore_signal(
            barrier, inc=1, device_id={"chan": lax.rem(me + offset, chans)}, device_id_type=MESH
        )

    @pl.when(not_first)
    def _():
        pl.semaphore_signal(barrier, inc=1, device_id={"slab": slab - 1}, device_id_type=MESH)

    @pl.when(not_last)
    def _():
        pl.semaphore_signal(barrier, inc=1, device_id={"slab": slab + 1}, device_id_type=MESH)

    source = lax.broadcasted_iota(jnp.int32, (2 * LANES, LANES), 0)
    lane = lax.broadcasted_iota(jnp.int32, (2 * LANES, LANES), 1)
    for copy in small:
        copy.wait()

    def put_band(kind, k, near):
        band[kind, k] = jnp.where(near, 1.0, 0.0).astype(jnp.bfloat16)

    target = jnp.where(lane < HALF, lane + LANES, lane)

    @pl.loop(0, MOMENTS)
    def _(k):
        put_band(0, k, jnp.abs(source - target) <= h_ref[k])

    def weight_copy(offset):
        return pltpu.make_async_remote_copy(
            src_ref=weights.at[0], dst_ref=weights.at[offset],
            send_sem=w_send.at[0], recv_sem=w_recv.at[offset - 1],
            device_id={"chan": lax.rem(me + offset, chans)}, device_id_type=MESH,
        )

    def pass_copy(hop, c):
        return pltpu.make_async_remote_copy(
            src_ref=sums.at[2 * hop, c], dst_ref=passed.at[hop, c],
            send_sem=pass_send.at[hop], recv_sem=pass_recv.at[hop, lax.rem(c, PASS_TURNS)],
            device_id={"chan": partner}, device_id_type=MESH,
        )

    def cross_copy(hop, c, k):
        other = lax.rem(group + hop + 1, groups) * 2 + core
        return pltpu.make_async_remote_copy(
            src_ref=sums.at[2 * hop + 1, c, k], dst_ref=crossed.at[hop, c, k],
            send_sem=cross_send.at[hop],
            recv_sem=cross_recv.at[hop, lax.rem(c, CROSS_TURNS), k],
            device_id={"chan": other}, device_id_type=MESH,
        )

    def up_copy(c, k):
        return pltpu.make_async_remote_copy(
            src_ref=ext.at[c, k, pl.ds(HW_MAX, HW_MAX)],
            dst_ref=ext.at[c, k, pl.ds(HW_MAX + rows, HW_MAX)],
            send_sem=up_send.at[0], recv_sem=up_recv.at[lax.rem(c, ROW_TURNS), k],
            device_id={"slab": slab - 1}, device_id_type=MESH,
        )

    def down_copy(c, k):
        return pltpu.make_async_remote_copy(
            src_ref=ext.at[c, k, pl.ds(rows, HW_MAX)],
            dst_ref=ext.at[c, k, pl.ds(0, HW_MAX)],
            send_sem=down_send.at[0], recv_sem=down_recv.at[lax.rem(c, ROW_TURNS), k],
            device_id={"slab": slab + 1}, device_id_type=MESH,
        )

    def moments_of(slot, tile):
        cols = pl.ds(pl.multiple_of((block_of(slot) * chunks + tile + 1) * LANES, LANES), LANES)

        @pl.loop(0, rows // ROWS_AT_ONCE)
        def _(part):
            first = pl.multiple_of(part * ROWS_AT_ONCE, ROWS_AT_ONCE)
            totals = [None] * MOMENTS
            for chan in range(local_chans):
                weight = w_ref[chan].astype(jnp.float32)
                offset = f_ref[chan]
                term = beams[tile, slot, chan, pl.ds(first, ROWS_AT_ONCE), :] * weight
                for k in range(MOMENTS):
                    if k > 0:
                        term = term * offset
                    totals[k] = term if chan == 0 else totals[k] + term
            for k in range(MOMENTS):
                for at, piece in enumerate(split(totals[k])):
                    pieces[k, pl.ds(first + at * rows, ROWS_AT_ONCE), cols] = piece

    def fold(product):
        result = product[:rows]
        for at in range(1, PARTS):
            result = result + product[at * rows : (at + 1) * rows]
        return result

    def lanes_from(slot, tile):
        first = (block_of(slot) * chunks + tile + 1) * LANES
        return pl.ds(pl.multiple_of(first, LANES), 2 * LANES)

    def columns_of(slot, c):
        wide = lanes_from(slot, c)
        for k in range(MOMENTS):
            sums[slot, c, k] = fold(
                jnp.dot(pieces[k, :, wide], band[0, k], preferred_element_type=jnp.float32)
            )

    def edge_of(slot):
        low, high = lanes_from(slot, -1), lanes_from(slot, chunks - 1)
        for k in range(MOMENTS):
            sums[slot, edge, k] = fold(
                jnp.dot(pieces[k, :, low], band[1, k], preferred_element_type=jnp.float32)
                + jnp.dot(pieces[k, :, high], band[2, k], preferred_element_type=jnp.float32)
            )

    def make(slot, c):
        if isinstance(c, int) and c == edge:
            edge_of(slot)
        else:
            moments_of(slot, c + 1)
            columns_of(slot, c)
        if slot % 2 == 0:
            pass_copy(slot // 2, c).start()

    def send_on(hop, c):
        pass_copy(hop, c).wait_recv()
        for k in range(MOMENTS):
            sums[2 * hop + 1, c, k] = sums[2 * hop + 1, c, k] + passed[hop, c, k]
            cross_copy(hop, c, k).start()

    def finish(c, k):
        value = sums[chans - 1, c, k] + passed[own, c, k]
        for hop in range(own):
            cross_copy(hop, c, k).wait_recv()
            value = value + crossed[hop, c, k]
        ext[c, k, HW_MAX : HW_MAX + rows, :] = value

        @pl.when(not_first)
        def _():
            up_copy(c, k).start()

        @pl.when(not_last)
        def _():
            down_copy(c, k).start()

    left = lax.broadcasted_iota(jnp.int32, (rows, LANES), 1) < HALF

    def rows_of(c, k):
        @pl.when(not_last)
        def _():
            up_copy(c, k).wait_recv()

        @pl.when(not_first)
        def _():
            down_copy(c, k).wait_recv()

        both = jnp.concatenate(split(ext[c, k]), axis=0)
        summed = jnp.dot(row_band[k], both, preferred_element_type=jnp.float32)
        summed = summed * scale[k, 0:1, :]
        if isinstance(c, int) and c == edge:
            at, to = slice(0, LANES), slice(edge * LANES, chunks * LANES)
            out_ref[k, :, at] = jnp.where(left, summed, out_ref[k, :, at])
            out_ref[k, :, to] = jnp.where(left, out_ref[k, :, to], summed)
        else:
            at = pl.ds(pl.multiple_of(c * LANES, LANES), LANES)
            to = pl.ds(pl.multiple_of((c + 1) * LANES, LANES), LANES)
            if isinstance(c, int) and c == 0:
                out_ref[k, :, at] = summed
            else:
                out_ref[k, :, at] = jnp.where(left, out_ref[k, :, at], summed)
            out_ref[k, :, to] = summed

    def start(slot):
        drain(beams.at[0:FIRST, slot], first_sem.at[slot])
        for tile in range(FIRST - 1):
            moments_of(slot, tile)
        make(slot, 0)

    drain(beams.at[0:FIRST, 0], first_sem.at[0])
    for tile in range(FIRST):
        moments_of(0, tile)
    columns_of(0, 0)
    pl.semaphore_wait(
        barrier, chans - 1 + not_first.astype(jnp.int32) + not_last.astype(jnp.int32)
    )
    pass_copy(0, 0).start()
    start(1)
    if own > 0:
        send_on(0, 0)

    total = w_ref[0].astype(jnp.float32)
    for chan in range(1, local_chans):
        total = total + w_ref[chan].astype(jnp.float32)
    weights[0] = jnp.full(weights.shape[1:], total, jnp.float32)
    for offset in range(1, chans):
        weight_copy(offset).start()

    for slot in range(2, chans):
        start(slot)
    for hop in range(1, own):
        send_on(hop, 0)
    drain(beams.at[FIRST], load_sem.at[0])
    for slot in range(chans):
        make(slot, 1)
    for hop in range(own):
        send_on(hop, 1)
    pass_copy(own, 0).wait_recv()

    @pl.when(slab == 0)
    def _():
        @pl.loop(0, chunks)
        def _(c):
            ext[c, :, 0:HW_MAX, :] = jnp.zeros((MOMENTS, HW_MAX, LANES), jnp.float32)

    @pl.when(slab == slabs - 1)
    def _():
        @pl.loop(0, chunks)
        def _(c):
            ext[c, :, HW_MAX + rows :, :] = jnp.zeros((MOMENTS, HW_MAX, LANES), jnp.float32)

    def set_rest():
        pieces[:, :, 0:LANES] = jnp.zeros(pieces.shape[:2] + (LANES,), jnp.bfloat16)
        pieces[:, :, LANES + all_cols :] = jnp.zeros(pieces.shape[:2] + (LANES,), jnp.bfloat16)
        for offset in range(1, chans):
            weight_copy(offset).wait_recv()
        weight_total = weights[0]
        for offset in range(1, chans):
            weight_total = weight_total + weights[offset]

        @pl.loop(0, MOMENTS)
        def _(k):
            reach = h_ref[k]
            near = jnp.logical_and(lane < HALF, jnp.abs(source - LANES - lane) <= reach)
            put_band(1, k, near)
            near = jnp.logical_and(lane >= HALF, jnp.abs(source - lane) <= reach)
            put_band(2, k, near)
            span = rows + 2 * HW_MAX
            to_row = lax.broadcasted_iota(jnp.int32, (rows, span), 0)
            from_row = lax.broadcasted_iota(jnp.int32, (rows, span), 1)
            near = jnp.abs(from_row - HW_MAX - to_row) <= reach
            near = jnp.where(near, 1.0, 0.0).astype(jnp.bfloat16)
            for part in range(PARTS):
                row_band[k, :, part * span : (part + 1) * span] = near
            divisor = weight_total * (2 * reach + 1).astype(jnp.float32)
            scale[k] = 1.0 / divisor

    def iteration(c, ahead, behind):
        jobs = []
        if ahead is not None:
            jobs = [functools.partial(make, slot, ahead) for slot in range(chans)]
            if not (isinstance(ahead, int) and ahead == edge):
                drain(beams.at[ahead + 1], load_sem.at[ahead + 1 - FIRST])
        for k in range(MOMENTS):
            finish(c, k)
            if k < MOMENTS - 1:
                share = -(-len(jobs) // (MOMENTS - 1 - k))
                for job in jobs[:share]:
                    job()
                jobs = jobs[share:]
            elif ahead is not None:
                for hop in range(own):
                    send_on(hop, ahead)
            if behind is not None:
                rows_of(behind, k)
        if not (isinstance(c, int) and c == edge):
            pass_copy(own, c + 1).wait_recv()

    iteration(0, 2, None)
    set_rest()
    iteration(1, 3, None)
    iteration(2, 4, 0)

    @pl.loop(3, edge - 2)
    def _(c):
        iteration(c, c + 2, c - 2)

    iteration(edge - 2, edge, edge - 4)
    iteration(edge - 1, None, edge - 3)
    iteration(edge, None, edge - 2)

    for k in range(MOMENTS):
        rows_of(edge - 1, k)

    for k in range(MOMENTS):
        rows_of(edge, k)

    drain(weights.at[1:chans], w_send.at[0])
    for hop in range(groups):
        drain(sums.at[2 * hop], pass_send.at[hop])
    for hop in range(own):
        drain(sums.at[2 * hop + 1], cross_send.at[hop])

    @pl.when(not_first)
    def _():
        drain(ext.at[:, :, HW_MAX : 2 * HW_MAX], up_send.at[0])

    @pl.when(not_last)
    def _():
        drain(ext.at[:, :, rows : rows + HW_MAX], down_send.at[0])


def body(chans, slabs, beam_images, chan_weights, freq_offsets, half_widths):
    local_chans, rows, all_cols = beam_images.shape
    width = all_cols // chans
    chunks, groups = width // LANES, chans // 2
    f32, b16 = jnp.float32, jnp.bfloat16
    dma = pltpu.SemaphoreType.DMA
    hbm = pl.BlockSpec(memory_space=pltpu.HBM)
    small = [
        pltpu.with_memory_space_constraint(value, pltpu.HBM)
        for value in (chan_weights, freq_offsets, half_widths)
    ]
    span = rows + 2 * HW_MAX
    return pl.pallas_call(
        functools.partial(kernel, chans, slabs),
        out_shape=jax.ShapeDtypeStruct((MOMENTS, rows, width), f32),
        in_specs=[hbm, hbm, hbm, hbm],
        out_specs=pl.BlockSpec(memory_space=pltpu.VMEM),
        scratch_shapes=[
            pltpu.SMEM(chan_weights.shape, jnp.int32),
            pltpu.SMEM(freq_offsets.shape, f32),
            pltpu.SMEM(half_widths.shape, jnp.int32),
            pltpu.VMEM((chunks, chans, local_chans, rows, LANES), f32),
            pltpu.VMEM((MOMENTS, PARTS * rows, all_cols + 2 * LANES), b16),
            pltpu.VMEM((3, MOMENTS, 2 * LANES, LANES), b16),
            pltpu.VMEM((MOMENTS, rows, PARTS * span), b16),
            pltpu.VMEM((chans, chunks, MOMENTS, rows, LANES), f32),
            pltpu.VMEM((groups, chunks, MOMENTS, rows, LANES), f32),
            pltpu.VMEM((groups - 1, chunks, MOMENTS, rows, LANES), f32),
            pltpu.VMEM((chunks, MOMENTS, span, LANES), f32),
            pltpu.VMEM((chans, 8, LANES), f32),
            pltpu.VMEM((MOMENTS, 8, LANES), f32),
            dma((3,)),
            dma((chans,)),
            dma((chunks - FIRST,)),
            dma((groups,)),
            dma((groups, PASS_TURNS)),
            dma((groups - 1,)),
            dma((groups - 1, CROSS_TURNS, MOMENTS)),
            dma((1,)),
            dma((ROW_TURNS, MOMENTS)),
            dma((1,)),
            dma((ROW_TURNS, MOMENTS)),
            dma((1,)),
            dma((chans - 1,)),
        ],
        compiler_params=pltpu.CompilerParams(
            collective_id=0, has_side_effects=True, vmem_limit_bytes=44 * 1024 * 1024
        ),
    )(*small, beam_images)


def solution(mesh):
    placed = (P("chan", "slab", None), P("chan"), P("chan"), P())
    return jax.shard_map(
        functools.partial(body, mesh.shape["chan"], mesh.shape["slab"]),
        mesh=mesh, in_specs=placed, out_specs=P(None, "slab", "chan"), check_vma=False,
    )
```

```python
import functools

import jax
import jax.numpy as jnp
from jax import lax
from jax.experimental import pallas as pl
from jax.experimental.pallas import tpu as pltpu
from jax.sharding import PartitionSpec as P

MOMENTS = 5
HW_MAX = 32
LANES = 128
HALF = LANES // 2
PARTS = 2
ROWS_AT_ONCE = 32
FIRST = 2
PASS_TURNS = 3
CROSS_TURNS = 4
ROW_TURNS = 5
MESH = pl.DeviceIdType.MESH


def split(value):
    parts = []
    for _ in range(PARTS - 1):
        part = value.astype(jnp.bfloat16)
        parts.append(part)
        value = value - part.astype(jnp.float32)
    parts.append(value.astype(jnp.bfloat16))
    return parts


def kernel(chans, slabs, *refs):
    chunks = refs[3].shape[2] // chans // LANES
    groups = chans // 2
    dma = pltpu.SemaphoreType.DMA
    pl.run_scoped(
        functools.partial(scoped, chans, slabs, *refs),
        dma((3,)),
        dma((chans, FIRST)),
        dma((chunks - FIRST,)),
        dma((groups,)),
        dma((groups, PASS_TURNS)),
        dma((groups - 1,)),
        dma((groups - 1, CROSS_TURNS, MOMENTS)),
        dma((1,)),
        dma((ROW_TURNS, MOMENTS)),
        dma((1,)),
        dma((ROW_TURNS, MOMENTS)),
        dma((1,)),
        dma((chans - 1,)),
    )


def scoped(
    chans, slabs,
    w_hbm, f_hbm, h_hbm, beam_ref, out_ref,
    w_ref, f_ref, h_ref,
    beams, pieces, band, row_band, sums, passed, crossed, ext, weights, scale,
    small_sem, first_sem, load_sem, pass_send, pass_recv, cross_send, cross_recv,
    up_send, up_recv, down_send, down_recv, w_send, w_recv,
):
    groups = chans // 2
    me = lax.axis_index("chan")
    slab = lax.axis_index("slab")
    group, core = me // 2, lax.rem(me, 2)
    local_chans, rows, all_cols = beam_ref.shape
    width = all_cols // chans
    chunks = width // LANES
    edge = chunks - 1
    own = groups - 1
    partner = group * 2 + (1 - core)
    not_first, not_last = slab > 0, slab < slabs - 1

    def block_of(slot):
        owner_group = lax.rem(group + slot // 2 + 1, groups)
        return owner_group * 2 + (1 - core if slot % 2 == 0 else core)

    def load(slot, tile):
        col = pl.multiple_of((block_of(slot) * chunks + tile) * LANES, LANES)
        sem = first_sem.at[slot, tile] if isinstance(tile, int) else load_sem.at[tile - FIRST]
        return pltpu.make_async_copy(
            beam_ref.at[:, :, pl.ds(col, LANES)], beams.at[tile, slot], sem
        )

    def drain(ref, sem):
        pltpu.make_async_copy(ref, ref, sem).wait()

    small = [
        pltpu.make_async_copy(source, target, small_sem.at[at])
        for at, (source, target) in enumerate(((h_hbm, h_ref), (w_hbm, w_ref), (f_hbm, f_ref)))
    ]
    for copy in small:
        copy.start()
    for slot in range(chans):
        for tile in range(FIRST):
            load(slot, tile).start()

    @pl.loop(FIRST, chunks)
    def _(tile):
        for slot in range(chans):
            load(slot, tile).start()

    barrier = pltpu.get_barrier_semaphore()
    for offset in range(1, chans):
        pl.semaphore_signal(
            barrier, inc=1, device_id={"chan": lax.rem(me + offset, chans)}, device_id_type=MESH
        )

    @pl.when(not_first)
    def _():
        pl.semaphore_signal(barrier, inc=1, device_id={"slab": slab - 1}, device_id_type=MESH)

    @pl.when(not_last)
    def _():
        pl.semaphore_signal(barrier, inc=1, device_id={"slab": slab + 1}, device_id_type=MESH)

    source = lax.broadcasted_iota(jnp.int32, (2 * LANES, LANES), 0)
    lane = lax.broadcasted_iota(jnp.int32, (2 * LANES, LANES), 1)
    for copy in small:
        copy.wait()

    def put_band(kind, k, near):
        band[kind, k] = jnp.where(near, 1.0, 0.0).astype(jnp.bfloat16)

    target = jnp.where(lane < HALF, lane + LANES, lane)

    @pl.loop(0, MOMENTS)
    def _(k):
        put_band(0, k, jnp.abs(source - target) <= h_ref[k])

    def weight_copy(offset):
        return pltpu.make_async_remote_copy(
            src_ref=weights.at[0], dst_ref=weights.at[offset],
            send_sem=w_send.at[0], recv_sem=w_recv.at[offset - 1],
            device_id={"chan": lax.rem(me + offset, chans)}, device_id_type=MESH,
        )

    def pass_copy(hop, c):
        return pltpu.make_async_remote_copy(
            src_ref=sums.at[2 * hop, c], dst_ref=passed.at[hop, c],
            send_sem=pass_send.at[hop], recv_sem=pass_recv.at[hop, lax.rem(c, PASS_TURNS)],
            device_id={"chan": partner}, device_id_type=MESH,
        )

    def cross_copy(hop, c, k):
        other = lax.rem(group + hop + 1, groups) * 2 + core
        return pltpu.make_async_remote_copy(
            src_ref=sums.at[2 * hop + 1, c, k], dst_ref=crossed.at[hop, c, k],
            send_sem=cross_send.at[hop],
            recv_sem=cross_recv.at[hop, lax.rem(c, CROSS_TURNS), k],
            device_id={"chan": other}, device_id_type=MESH,
        )

    def up_copy(c, k):
        return pltpu.make_async_remote_copy(
            src_ref=ext.at[c, k, pl.ds(HW_MAX, HW_MAX)],
            dst_ref=ext.at[c, k, pl.ds(HW_MAX + rows, HW_MAX)],
            send_sem=up_send.at[0], recv_sem=up_recv.at[lax.rem(c, ROW_TURNS), k],
            device_id={"slab": slab - 1}, device_id_type=MESH,
        )

    def down_copy(c, k):
        return pltpu.make_async_remote_copy(
            src_ref=ext.at[c, k, pl.ds(rows, HW_MAX)],
            dst_ref=ext.at[c, k, pl.ds(0, HW_MAX)],
            send_sem=down_send.at[0], recv_sem=down_recv.at[lax.rem(c, ROW_TURNS), k],
            device_id={"slab": slab + 1}, device_id_type=MESH,
        )

    def moments_of(slot, tile):
        cols = pl.ds(pl.multiple_of((block_of(slot) * chunks + tile + 1) * LANES, LANES), LANES)

        @pl.loop(0, rows // ROWS_AT_ONCE)
        def _(part):
            first = pl.multiple_of(part * ROWS_AT_ONCE, ROWS_AT_ONCE)
            totals = [None] * MOMENTS
            for chan in range(local_chans):
                weight = w_ref[chan].astype(jnp.float32)
                offset = f_ref[chan]
                term = beams[tile, slot, chan, pl.ds(first, ROWS_AT_ONCE), :] * weight
                for k in range(MOMENTS):
                    if k > 0:
                        term = term * offset
                    totals[k] = term if chan == 0 else totals[k] + term
            for k in range(MOMENTS):
                for at, piece in enumerate(split(totals[k])):
                    pieces[k, pl.ds(first + at * rows, ROWS_AT_ONCE), cols] = piece

    def fold(product):
        result = product[:rows]
        for at in range(1, PARTS):
            result = result + product[at * rows : (at + 1) * rows]
        return result

    def lanes_from(slot, tile):
        first = (block_of(slot) * chunks + tile + 1) * LANES
        return pl.ds(pl.multiple_of(first, LANES), 2 * LANES)

    def columns_of(slot, c):
        wide = lanes_from(slot, c)
        for k in range(MOMENTS):
            sums[slot, c, k] = fold(
                jnp.dot(pieces[k, :, wide], band[0, k], preferred_element_type=jnp.float32)
            )

    def edge_of(slot):
        low, high = lanes_from(slot, -1), lanes_from(slot, chunks - 1)
        for k in range(MOMENTS):
            sums[slot, edge, k] = fold(
                jnp.dot(pieces[k, :, low], band[1, k], preferred_element_type=jnp.float32)
                + jnp.dot(pieces[k, :, high], band[2, k], preferred_element_type=jnp.float32)
            )

    def make(slot, c):
        if isinstance(c, int) and c == edge:
            edge_of(slot)
        else:
            moments_of(slot, c + 1)
            columns_of(slot, c)
        if slot % 2 == 0:
            pass_copy(slot // 2, c).start()

    def send_on(hop, c):
        pass_copy(hop, c).wait_recv()
        for k in range(MOMENTS):
            sums[2 * hop + 1, c, k] = sums[2 * hop + 1, c, k] + passed[hop, c, k]
            cross_copy(hop, c, k).start()

    def finish(c, k):
        value = sums[chans - 1, c, k] + passed[own, c, k]
        for hop in range(own):
            cross_copy(hop, c, k).wait_recv()
            value = value + crossed[hop, c, k]
        ext[c, k, HW_MAX : HW_MAX + rows, :] = value

        @pl.when(not_first)
        def _():
            up_copy(c, k).start()

        @pl.when(not_last)
        def _():
            down_copy(c, k).start()

    left = lax.broadcasted_iota(jnp.int32, (rows, LANES), 1) < HALF

    def rows_of(c, k):
        @pl.when(not_last)
        def _():
            up_copy(c, k).wait_recv()

        @pl.when(not_first)
        def _():
            down_copy(c, k).wait_recv()

        both = jnp.concatenate(split(ext[c, k]), axis=0)
        summed = jnp.dot(row_band[k], both, preferred_element_type=jnp.float32)
        summed = summed * scale[k, 0:1, :]
        if isinstance(c, int) and c == edge:
            at, to = slice(0, LANES), slice(edge * LANES, chunks * LANES)
            out_ref[k, :, at] = jnp.where(left, summed, out_ref[k, :, at])
            out_ref[k, :, to] = jnp.where(left, out_ref[k, :, to], summed)
        else:
            at = pl.ds(pl.multiple_of(c * LANES, LANES), LANES)
            to = pl.ds(pl.multiple_of((c + 1) * LANES, LANES), LANES)
            if isinstance(c, int) and c == 0:
                out_ref[k, :, at] = summed
            else:
                out_ref[k, :, at] = jnp.where(left, out_ref[k, :, at], summed)
            out_ref[k, :, to] = summed

    def start(slot):
        for tile in range(FIRST):
            load(slot, tile).wait()
            moments_of(slot, tile)
        columns_of(slot, 0)

    start(0)
    pl.semaphore_wait(
        barrier, chans - 1 + not_first.astype(jnp.int32) + not_last.astype(jnp.int32)
    )
    pass_copy(0, 0).start()
    start(1)
    if own > 0:
        send_on(0, 0)

    total = w_ref[0].astype(jnp.float32)
    for chan in range(1, local_chans):
        total = total + w_ref[chan].astype(jnp.float32)
    weights[0] = jnp.full(weights.shape[1:], total, jnp.float32)
    for offset in range(1, chans):
        weight_copy(offset).start()

    for slot in range(2, chans):
        start(slot)
        if slot % 2 == 0:
            pass_copy(slot // 2, 0).start()
    for hop in range(1, own):
        send_on(hop, 0)
    drain(beams.at[FIRST], load_sem.at[0])
    for slot in range(chans):
        make(slot, 1)
    for hop in range(own):
        send_on(hop, 1)
    pass_copy(own, 0).wait_recv()

    @pl.when(slab == 0)
    def _():
        @pl.loop(0, chunks)
        def _(c):
            ext[c, :, 0:HW_MAX, :] = jnp.zeros((MOMENTS, HW_MAX, LANES), jnp.float32)

    @pl.when(slab == slabs - 1)
    def _():
        @pl.loop(0, chunks)
        def _(c):
            ext[c, :, HW_MAX + rows :, :] = jnp.zeros((MOMENTS, HW_MAX, LANES), jnp.float32)

    def set_rest():
        pieces[:, :, 0:LANES] = jnp.zeros(pieces.shape[:2] + (LANES,), jnp.bfloat16)
        pieces[:, :, LANES + all_cols :] = jnp.zeros(pieces.shape[:2] + (LANES,), jnp.bfloat16)
        for offset in range(1, chans):
            weight_copy(offset).wait_recv()
        weight_total = weights[0]
        for offset in range(1, chans):
            weight_total = weight_total + weights[offset]

        @pl.loop(0, MOMENTS)
        def _(k):
            reach = h_ref[k]
            near = jnp.logical_and(lane < HALF, jnp.abs(source - LANES - lane) <= reach)
            put_band(1, k, near)
            near = jnp.logical_and(lane >= HALF, jnp.abs(source - lane) <= reach)
            put_band(2, k, near)
            span = rows + 2 * HW_MAX
            to_row = lax.broadcasted_iota(jnp.int32, (rows, span), 0)
            from_row = lax.broadcasted_iota(jnp.int32, (rows, span), 1)
            near = jnp.abs(from_row - HW_MAX - to_row) <= reach
            near = jnp.where(near, 1.0, 0.0).astype(jnp.bfloat16)
            for part in range(PARTS):
                row_band[k, :, part * span : (part + 1) * span] = near
            divisor = weight_total * (2 * reach + 1).astype(jnp.float32)
            scale[k] = 1.0 / divisor

    def iteration(c, ahead, behind):
        jobs = []
        if ahead is not None:
            jobs = [functools.partial(make, slot, ahead) for slot in range(chans)]
            if not (isinstance(ahead, int) and ahead == edge):
                drain(beams.at[ahead + 1], load_sem.at[ahead + 1 - FIRST])
        for k in range(MOMENTS):
            finish(c, k)
            if k < MOMENTS - 1:
                share = -(-len(jobs) // (MOMENTS - 1 - k))
                for job in jobs[:share]:
                    job()
                jobs = jobs[share:]
            elif ahead is not None:
                for hop in range(own):
                    send_on(hop, ahead)
            if behind is not None:
                rows_of(behind, k)
        if not (isinstance(c, int) and c == edge):
            pass_copy(own, c + 1).wait_recv()

    iteration(0, 2, None)
    set_rest()
    iteration(1, 3, None)
    iteration(2, 4, 0)

    @pl.loop(3, edge - 2)
    def _(c):
        iteration(c, c + 2, c - 2)

    iteration(edge - 2, edge, edge - 4)
    iteration(edge - 1, None, edge - 3)
    iteration(edge, None, edge - 2)

    for k in range(MOMENTS):
        rows_of(edge - 1, k)

    for k in range(MOMENTS):
        rows_of(edge, k)

    drain(weights.at[1:chans], w_send.at[0])
    for hop in range(groups):
        drain(sums.at[2 * hop], pass_send.at[hop])
    for hop in range(own):
        drain(sums.at[2 * hop + 1], cross_send.at[hop])

    @pl.when(not_first)
    def _():
        drain(ext.at[:, :, HW_MAX : 2 * HW_MAX], up_send.at[0])

    @pl.when(not_last)
    def _():
        drain(ext.at[:, :, rows : rows + HW_MAX], down_send.at[0])


def body(chans, slabs, beam_images, chan_weights, freq_offsets, half_widths):
    local_chans, rows, all_cols = beam_images.shape
    width = all_cols // chans
    chunks, groups = width // LANES, chans // 2
    f32, b16 = jnp.float32, jnp.bfloat16
    hbm = pl.BlockSpec(memory_space=pltpu.HBM)
    small = [
        pltpu.with_memory_space_constraint(value, pltpu.HBM)
        for value in (chan_weights, freq_offsets, half_widths)
    ]
    span = rows + 2 * HW_MAX
    return pl.pallas_call(
        functools.partial(kernel, chans, slabs),
        out_shape=jax.ShapeDtypeStruct((MOMENTS, rows, width), f32),
        in_specs=[hbm, hbm, hbm, hbm],
        out_specs=pl.BlockSpec(memory_space=pltpu.VMEM),
        scratch_shapes=[
            pltpu.SMEM(chan_weights.shape, jnp.int32),
            pltpu.SMEM(freq_offsets.shape, f32),
            pltpu.SMEM(half_widths.shape, jnp.int32),
            pltpu.VMEM((chunks, chans, local_chans, rows, LANES), f32),
            pltpu.VMEM((MOMENTS, PARTS * rows, all_cols + 2 * LANES), b16),
            pltpu.VMEM((3, MOMENTS, 2 * LANES, LANES), b16),
            pltpu.VMEM((MOMENTS, rows, PARTS * span), b16),
            pltpu.VMEM((chans, chunks, MOMENTS, rows, LANES), f32),
            pltpu.VMEM((groups, chunks, MOMENTS, rows, LANES), f32),
            pltpu.VMEM((groups - 1, chunks, MOMENTS, rows, LANES), f32),
            pltpu.VMEM((chunks, MOMENTS, span, LANES), f32),
            pltpu.VMEM((chans, 8, LANES), f32),
            pltpu.VMEM((MOMENTS, 8, LANES), f32),
        ],
        compiler_params=pltpu.CompilerParams(
            collective_id=0, has_side_effects=True, vmem_limit_bytes=44 * 1024 * 1024
        ),
    )(*small, beam_images)


def solution(mesh):
    placed = (P("chan", "slab", None), P("chan"), P("chan"), P())
    return jax.shard_map(
        functools.partial(body, mesh.shape["chan"], mesh.shape["slab"]),
        mesh=mesh, in_specs=placed, out_specs=P(None, "slab", "chan"), check_vma=False,
    )
```

```python
import functools

import jax
import jax.numpy as jnp
from jax import lax
from jax.experimental import pallas as pl
from jax.experimental.pallas import tpu as pltpu
from jax.sharding import PartitionSpec as P

MOMENTS = 5
HW_MAX = 32
LANES = 128
HALF = LANES // 2
PARTS = 2
ROWS_AT_ONCE = 32
FIRST = 2
LATE = 2
LATE_AT = 3
HALVES = 2
MESH = pl.DeviceIdType.MESH


def split(value):
    parts = []
    for _ in range(PARTS - 1):
        part = value.astype(jnp.bfloat16)
        parts.append(part)
        value = value - part.astype(jnp.float32)
    parts.append(value.astype(jnp.bfloat16))
    return parts


def kernel(chans, slabs, *refs):
    chunks = refs[3].shape[2] // chans // LANES
    groups = chans // 2
    dma = pltpu.SemaphoreType.DMA
    pl.run_scoped(
        functools.partial(scoped, chans, slabs, *refs),
        dma((3,)),
        dma((chans, FIRST)),
        dma((chunks - FIRST,)),
        dma((groups,)),
        dma((groups, chunks)),
        dma((groups - 1,)),
        dma((groups - 1, chunks, MOMENTS, HALVES)),
        dma((1,)),
        dma((chunks * MOMENTS + (groups - 1) * LATE,)),
        dma((1,)),
        dma((chunks * MOMENTS + (groups - 1) * LATE,)),
        dma((1,)),
        dma((chans - 1,)),
    )


def scoped(
    chans, slabs,
    w_hbm, f_hbm, h_hbm, beam_ref, out_ref,
    w_ref, f_ref, h_ref,
    beams, pieces, band, row_band, sums, passed, crossed, ext, late, weights, scale,
    small_sem, first_sem, load_sem, pass_send, pass_recv, cross_send, cross_recv,
    up_send, up_recv, down_send, down_recv, w_send, w_recv,
):
    groups = chans // 2
    me = lax.axis_index("chan")
    slab = lax.axis_index("slab")
    group, core = me // 2, lax.rem(me, 2)
    local_chans, rows, all_cols = beam_ref.shape
    width = all_cols // chans
    chunks = width // LANES
    edge = chunks - 1
    own = groups - 1
    partner = group * 2 + (1 - core)
    not_first, not_last = slab > 0, slab < slabs - 1

    def block_of(slot):
        owner_group = lax.rem(group + slot // 2 + 1, groups)
        return owner_group * 2 + (1 - core if slot % 2 == 0 else core)

    def load(slot, tile):
        col = pl.multiple_of((block_of(slot) * chunks + tile) * LANES, LANES)
        sem = first_sem.at[slot, tile] if isinstance(tile, int) else load_sem.at[tile - FIRST]
        return pltpu.make_async_copy(
            beam_ref.at[:, :, pl.ds(col, LANES)], beams.at[tile, slot], sem
        )

    def drain(ref, sem):
        pltpu.make_async_copy(ref, ref, sem).wait()

    barrier = pltpu.get_barrier_semaphore()
    for offset in range(1, chans):
        pl.semaphore_signal(
            barrier, inc=1, device_id={"chan": lax.rem(me + offset, chans)}, device_id_type=MESH
        )

    @pl.when(not_first)
    def _():
        pl.semaphore_signal(barrier, inc=1, device_id={"slab": slab - 1}, device_id_type=MESH)

    @pl.when(not_last)
    def _():
        pl.semaphore_signal(barrier, inc=1, device_id={"slab": slab + 1}, device_id_type=MESH)

    small = [
        pltpu.make_async_copy(source, target, small_sem.at[at])
        for at, (source, target) in enumerate(((h_hbm, h_ref), (w_hbm, w_ref), (f_hbm, f_ref)))
    ]
    for copy in small:
        copy.start()
    for slot in range(chans):
        for tile in range(FIRST):
            load(slot, tile).start()

    @pl.loop(FIRST, chunks)
    def _(tile):
        for slot in range(chans):
            load(slot, tile).start()

    source = lax.broadcasted_iota(jnp.int32, (2 * LANES, LANES), 0)
    lane = lax.broadcasted_iota(jnp.int32, (2 * LANES, LANES), 1)
    for copy in small:
        copy.wait()

    def put_band(kind, k, near):
        band[kind, k] = jnp.where(near, 1.0, 0.0).astype(jnp.bfloat16)

    target = jnp.where(lane < HALF, lane + LANES, lane)

    @pl.loop(0, MOMENTS)
    def _(k):
        put_band(0, k, jnp.abs(source - target) <= h_ref[k])

    def weight_copy(offset):
        return pltpu.make_async_remote_copy(
            src_ref=weights.at[0], dst_ref=weights.at[offset],
            send_sem=w_send.at[0], recv_sem=w_recv.at[offset - 1],
            device_id={"chan": lax.rem(me + offset, chans)}, device_id_type=MESH,
        )

    def pass_copy(hop, c):
        return pltpu.make_async_remote_copy(
            src_ref=sums.at[2 * hop, c], dst_ref=passed.at[hop, c],
            send_sem=pass_send.at[hop], recv_sem=pass_recv.at[hop, c],
            device_id={"chan": partner}, device_id_type=MESH,
        )

    def other(hop):
        return lax.rem(group + hop + 1, groups) * 2 + core

    def cross_copy(hop, c, k, half):
        part = pl.ds(half * rows // HALVES, rows // HALVES)
        return pltpu.make_async_remote_copy(
            src_ref=sums.at[2 * hop + 1, c, k, part], dst_ref=crossed.at[hop, c, k, part],
            send_sem=cross_send.at[hop], recv_sem=cross_recv.at[hop, c, k, half],
            device_id={"chan": other(hop)}, device_id_type=MESH,
        )

    def late_copy(hop, j):
        return pltpu.make_async_remote_copy(
            src_ref=late.at[hop, j], dst_ref=crossed.at[hop, 0, MOMENTS - LATE + j],
            send_sem=cross_send.at[hop], recv_sem=cross_recv.at[hop, 0, MOMENTS - LATE + j, 0],
            device_id={"chan": other(hop)}, device_id_type=MESH,
        )

    def place(c, k):
        return c * MOMENTS + k

    def late_place(hop, j):
        if hop == own:
            return place(0, MOMENTS - LATE + j)
        return chunks * MOMENTS + hop * LATE + j

    def up_copy(at):
        return pltpu.make_async_remote_copy(
            src_ref=ext.at[at, pl.ds(HW_MAX, HW_MAX)],
            dst_ref=ext.at[at, pl.ds(HW_MAX + rows, HW_MAX)],
            send_sem=up_send.at[0], recv_sem=up_recv.at[at],
            device_id={"slab": slab - 1}, device_id_type=MESH,
        )

    def down_copy(at):
        return pltpu.make_async_remote_copy(
            src_ref=ext.at[at, pl.ds(rows, HW_MAX)],
            dst_ref=ext.at[at, pl.ds(0, HW_MAX)],
            send_sem=down_send.at[0], recv_sem=down_recv.at[at],
            device_id={"slab": slab + 1}, device_id_type=MESH,
        )

    def moments_of(slot, tile):
        cols = pl.ds(pl.multiple_of((block_of(slot) * chunks + tile + 1) * LANES, LANES), LANES)

        for first in range(0, rows, ROWS_AT_ONCE):
            totals = [None] * MOMENTS
            for chan in range(local_chans):
                weight = w_ref[chan].astype(jnp.float32)
                offset = f_ref[chan]
                term = beams[tile, slot, chan, pl.ds(first, ROWS_AT_ONCE), :] * weight
                for k in range(MOMENTS):
                    if k > 0:
                        term = term * offset
                    totals[k] = term if chan == 0 else totals[k] + term
            for k in range(MOMENTS):
                for at, piece in enumerate(split(totals[k])):
                    pieces[k, pl.ds(first + at * rows, ROWS_AT_ONCE), cols] = piece

    def fold(product):
        result = product[:rows]
        for at in range(1, PARTS):
            result = result + product[at * rows : (at + 1) * rows]
        return result

    def lanes_from(slot, tile):
        first = (block_of(slot) * chunks + tile + 1) * LANES
        return pl.ds(pl.multiple_of(first, LANES), 2 * LANES)

    def columns_of(slot, c):
        wide = lanes_from(slot, c)
        for k in range(MOMENTS):
            sums[slot, c, k] = fold(
                jnp.dot(pieces[k, :, wide], band[0, k], preferred_element_type=jnp.float32)
            )

    def edge_of(slot):
        low, high = lanes_from(slot, -1), lanes_from(slot, chunks - 1)
        for k in range(MOMENTS):
            sums[slot, edge, k] = fold(
                jnp.dot(pieces[k, :, low], band[1, k], preferred_element_type=jnp.float32)
                + jnp.dot(pieces[k, :, high], band[2, k], preferred_element_type=jnp.float32)
            )

    def make(slot, c, following=()):
        if isinstance(c, int) and c == edge:
            edge_of(slot)
        else:
            columns_of(slot, c)
        for other_slot, tile in following:
            moments_of(other_slot, tile)
        if slot % 2 == 0:
            pass_copy(slot // 2, c).start()

    def makes(c):
        jobs = []
        for slot in range(chans):
            if isinstance(c, int) and c == edge:
                following = ()
            elif slot < chans - 1:
                following = ((slot + 1, c + 1),)
            elif isinstance(c, int) and c == edge - 1:
                following = ()
            else:
                following = ((0, c + 2),)
            jobs.append(functools.partial(make, slot, c, following))
        return jobs

    def crosses(c, k):
        return not (isinstance(c, int) and c == 0 and k >= MOMENTS - LATE)

    def send_on(hop, c):
        pass_copy(hop, c).wait_recv()
        for k in range(MOMENTS):
            value = sums[2 * hop + 1, c, k] + passed[hop, c, k]
            if crosses(c, k):
                sums[2 * hop + 1, c, k] = value
                for half in range(HALVES):
                    cross_copy(hop, c, k, half).start()
            else:
                share(late_place(hop, k - MOMENTS + LATE), value)

    def send_up(at):
        @pl.when(not_first)
        def _():
            up_copy(at).start()

    def send_down(at):
        @pl.when(not_last)
        def _():
            down_copy(at).start()

    def share(at, value):
        ext[at, HW_MAX : HW_MAX + rows, :] = value
        send_up(at)
        send_down(at)

    def finish(c, k):
        at = place(c, k)
        for half in range(HALVES):
            first, count = half * rows // HALVES, rows // HALVES
            part = slice(first, first + count)
            value = sums[chans - 1, c, k, part] + passed[own, c, k, part]
            for hop in range(own):
                cross_copy(hop, c, k, half).wait_recv()
                value = value + crossed[hop, c, k, part]
            ext[at, HW_MAX + first : HW_MAX + first + count, :] = value
            if half == 0 and HALVES == 2:
                send_up(at)
        if HALVES == 1:
            send_up(at)
        send_down(at)

    left = lax.broadcasted_iota(jnp.int32, (rows, LANES), 1) < HALF

    def row_sums(at, k):
        @pl.when(not_last)
        def _():
            up_copy(at).wait_recv()

        @pl.when(not_first)
        def _():
            down_copy(at).wait_recv()

        both = jnp.concatenate(split(ext[at]), axis=0)
        return jnp.dot(row_band[k], both, preferred_element_type=jnp.float32)

    def rows_of(c, k):
        if not crosses(c, k):
            return
        summed = row_sums(place(c, k), k) * scale[k, 0:1, :]
        if isinstance(c, int) and c == edge:
            at, to = slice(0, LANES), slice(edge * LANES, chunks * LANES)
            out_ref[k, :, at] = jnp.where(left, summed, out_ref[k, :, at])
            out_ref[k, :, to] = jnp.where(left, out_ref[k, :, to], summed)
        else:
            at = pl.ds(pl.multiple_of(c * LANES, LANES), LANES)
            to = pl.ds(pl.multiple_of((c + 1) * LANES, LANES), LANES)
            if isinstance(c, int) and c == 0:
                out_ref[k, :, at] = summed
            else:
                out_ref[k, :, at] = jnp.where(left, out_ref[k, :, at], summed)
            out_ref[k, :, to] = summed

    def late_rows(hop):
        for j in range(LATE):
            late[hop, j] = row_sums(late_place(hop, j), MOMENTS - LATE + j)

    def late_out(j):
        k = MOMENTS - LATE + j
        summed = late[own, j]
        for hop in range(own):
            late_copy(hop, j).wait_recv()
            summed = summed + crossed[hop, 0, k]
        summed = summed * scale[k, 0:1, :]
        out_ref[k, :, 0:LANES] = summed
        out_ref[k, :, LANES : 2 * LANES] = jnp.where(
            left, summed, out_ref[k, :, LANES : 2 * LANES]
        )

    @pl.when(slab == 0)
    def _():
        @pl.loop(0, ext.shape[0])
        def _(at):
            ext[at, 0:HW_MAX, :] = jnp.zeros((HW_MAX, LANES), jnp.float32)

    @pl.when(slab == slabs - 1)
    def _():
        @pl.loop(0, ext.shape[0])
        def _(at):
            ext[at, HW_MAX + rows :, :] = jnp.zeros((HW_MAX, LANES), jnp.float32)

    for tile in range(FIRST):
        load(0, tile).wait()
        moments_of(0, tile)
    columns_of(0, 0)
    pl.semaphore_wait(
        barrier, chans - 1 + not_first.astype(jnp.int32) + not_last.astype(jnp.int32)
    )
    pass_copy(0, 0).start()
    for slot in range(1, 2 * own):
        for tile in range(FIRST):
            load(slot, tile).wait()
            if slot % 2 == 1 or tile > 0:
                moments_of(slot, tile)
        if slot % 2 == 1:
            load(slot + 1, 0).wait()
            make(slot, 0, ((slot + 1, 0),))
            send_on(slot // 2, 0)
        else:
            make(slot, 0)

    total = w_ref[0].astype(jnp.float32)
    for chan in range(1, local_chans):
        total = total + w_ref[chan].astype(jnp.float32)
    weights[0] = jnp.full(weights.shape[1:], total, jnp.float32)
    for offset in range(1, chans):
        weight_copy(offset).start()

    load(2 * own, 1).wait()
    moments_of(2 * own, 1)
    for tile in range(FIRST):
        load(chans - 1, tile).wait()
    make(2 * own, 0, tuple((chans - 1, tile) for tile in range(FIRST)))
    drain(beams.at[FIRST], load_sem.at[0])
    make(chans - 1, 0, ((0, FIRST),))
    jobs = makes(1)
    for job in jobs[:-1]:
        job()
    pass_copy(own, 0).wait_recv()
    for j in range(LATE):
        k = MOMENTS - LATE + j
        share(late_place(own, j), sums[chans - 1, 0, k] + passed[own, 0, k])
    drain(beams.at[FIRST + 1], load_sem.at[1])
    jobs[-1]()
    for hop in range(own):
        send_on(hop, 1)

    def set_rest():
        out_ref[MOMENTS - LATE :, :, LANES : 2 * LANES] = jnp.zeros((LATE, rows, LANES), jnp.float32)
        pieces[:, :, 0:LANES] = jnp.zeros(pieces.shape[:2] + (LANES,), jnp.bfloat16)
        pieces[:, :, LANES + all_cols :] = jnp.zeros(pieces.shape[:2] + (LANES,), jnp.bfloat16)
        for offset in range(1, chans):
            weight_copy(offset).wait_recv()
        weight_total = weights[0]
        for offset in range(1, chans):
            weight_total = weight_total + weights[offset]

        @pl.loop(0, MOMENTS)
        def _(k):
            reach = h_ref[k]
            near = jnp.logical_and(lane < HALF, jnp.abs(source - LANES - lane) <= reach)
            put_band(1, k, near)
            near = jnp.logical_and(lane >= HALF, jnp.abs(source - lane) <= reach)
            put_band(2, k, near)
            span = rows + 2 * HW_MAX
            to_row = lax.broadcasted_iota(jnp.int32, (rows, span), 0)
            from_row = lax.broadcasted_iota(jnp.int32, (rows, span), 1)
            near = jnp.abs(from_row - HW_MAX - to_row) <= reach
            near = jnp.where(near, 1.0, 0.0).astype(jnp.bfloat16)
            for part in range(PARTS):
                row_band[k, :, part * span : (part + 1) * span] = near
            divisor = weight_total * (2 * reach + 1).astype(jnp.float32)
            scale[k] = 1.0 / divisor

    def fetch(tile):
        if not (isinstance(tile, int) and tile >= chunks):
            drain(beams.at[tile], load_sem.at[tile - FIRST])

    def iteration(c, ahead, behind):
        jobs = []
        if ahead is not None:
            jobs = makes(ahead)
            fetch(ahead + 2)
        for k in range(MOMENTS):
            if crosses(c, k):
                finish(c, k)
            if k < MOMENTS - 1:
                share = -(-len(jobs) // (MOMENTS - 1 - k))
                for job in jobs[:share]:
                    job()
                jobs = jobs[share:]
            elif ahead is not None:
                for hop in range(own):
                    send_on(hop, ahead)
            if isinstance(c, int) and c == edge and k == LATE_AT:
                for hop in range(own):
                    for j in range(LATE):
                        late_copy(hop, j).start()
            if behind is not None:
                rows_of(behind, k)
        if not (isinstance(c, int) and c == edge):
            pass_copy(own, c + 1).wait_recv()

    iteration(0, 2, None)
    set_rest()
    iteration(1, 3, None)
    for hop in range(groups):
        late_rows(hop)
    iteration(2, 4, 0)

    @pl.loop(3, edge - 3)
    def _(c):
        iteration(c, c + 2, c - 2)

    iteration(edge - 3, edge - 1, edge - 5)
    iteration(edge - 2, edge, edge - 4)
    iteration(edge - 1, None, edge - 3)
    iteration(edge, None, edge - 2)
    for k in range(MOMENTS):
        rows_of(edge - 1, k)
    drain(weights.at[1:chans], w_send.at[0])
    for hop in range(groups):
        drain(sums.at[2 * hop], pass_send.at[hop])
    for j in range(LATE):
        late_out(j)
    for k in range(MOMENTS):
        rows_of(edge, k)
    for hop in range(own):
        drain(sums.at[2 * hop + 1], cross_send.at[hop])

    @pl.when(not_first)
    def _():
        drain(ext.at[:, HW_MAX : 2 * HW_MAX], up_send.at[0])

    @pl.when(not_last)
    def _():
        drain(ext.at[:, rows : rows + HW_MAX], down_send.at[0])


def body(chans, slabs, beam_images, chan_weights, freq_offsets, half_widths):
    local_chans, rows, all_cols = beam_images.shape
    width = all_cols // chans
    chunks, groups = width // LANES, chans // 2
    f32, b16 = jnp.float32, jnp.bfloat16
    hbm = pl.BlockSpec(memory_space=pltpu.HBM)
    small = [
        pltpu.with_memory_space_constraint(value, pltpu.HBM)
        for value in (chan_weights, freq_offsets, half_widths)
    ]
    span = rows + 2 * HW_MAX
    return pl.pallas_call(
        functools.partial(kernel, chans, slabs),
        out_shape=jax.ShapeDtypeStruct((MOMENTS, rows, width), f32),
        in_specs=[hbm, hbm, hbm, hbm],
        out_specs=pl.BlockSpec(memory_space=pltpu.VMEM),
        scratch_shapes=[
            pltpu.SMEM(chan_weights.shape, jnp.int32),
            pltpu.SMEM(freq_offsets.shape, f32),
            pltpu.SMEM(half_widths.shape, jnp.int32),
            pltpu.VMEM((chunks, chans, local_chans, rows, LANES), f32),
            pltpu.VMEM((MOMENTS, PARTS * rows, all_cols + 2 * LANES), b16),
            pltpu.VMEM((3, MOMENTS, 2 * LANES, LANES), b16),
            pltpu.VMEM((MOMENTS, rows, PARTS * span), b16),
            pltpu.VMEM((chans, chunks, MOMENTS, rows, LANES), f32),
            pltpu.VMEM((groups, chunks, MOMENTS, rows, LANES), f32),
            pltpu.VMEM((groups - 1, chunks, MOMENTS, rows, LANES), f32),
            pltpu.VMEM((chunks * MOMENTS + (groups - 1) * LATE, span, LANES), f32),
            pltpu.VMEM((groups, LATE, rows, LANES), f32),
            pltpu.VMEM((chans, 8, LANES), f32),
            pltpu.VMEM((MOMENTS, 8, LANES), f32),
        ],
        compiler_params=pltpu.CompilerParams(
            collective_id=0, has_side_effects=True, vmem_limit_bytes=44 * 1024 * 1024
        ),
    )(*small, beam_images)


def solution(mesh):
    placed = (P("chan", "slab", None), P("chan"), P("chan"), P())
    return jax.shard_map(
        functools.partial(body, mesh.shape["chan"], mesh.shape["slab"]),
        mesh=mesh, in_specs=placed, out_specs=P(None, "slab", "chan"), check_vma=False,
    )
```

```python
import functools

import jax
import jax.numpy as jnp
from jax import lax
from jax.experimental import pallas as pl
from jax.experimental.pallas import tpu as pltpu
from jax.sharding import PartitionSpec as P

MOMENTS = 5
HW_MAX = 32
LANES = 128
HALF = LANES // 2
PARTS = 2
ROWS_AT_ONCE = 32
FIRST = 3
LATE = 3
LATE_AT = 2
TAIL = 1
HALVES = 2
MESH = pl.DeviceIdType.MESH


def split(value):
    parts = []
    for _ in range(PARTS - 1):
        part = value.astype(jnp.bfloat16)
        parts.append(part)
        value = value - part.astype(jnp.float32)
    parts.append(value.astype(jnp.bfloat16))
    return parts


def kernel(chans, slabs, *refs):
    chunks = refs[3].shape[2] // chans // LANES
    groups = chans // 2
    dma = pltpu.SemaphoreType.DMA
    pl.run_scoped(
        functools.partial(scoped, chans, slabs, *refs),
        dma((3,)),
        dma((chans, FIRST)),
        dma((chunks - FIRST,)),
        dma((groups,)),
        dma((groups, chunks)),
        dma((groups - 1,)),
        dma((groups - 1, chunks, MOMENTS, HALVES)),
        dma((1,)),
        dma((chunks * MOMENTS + (groups - 1) * LATE,)),
        dma((1,)),
        dma((chunks * MOMENTS + (groups - 1) * LATE,)),
        dma((1,)),
        dma((chans - 1,)),
    )


def scoped(
    chans, slabs,
    w_hbm, f_hbm, h_hbm, beam_ref, out_ref,
    w_ref, f_ref, h_ref,
    beams, pieces, band, row_band, sums, passed, crossed, ext, late, weights, scale,
    small_sem, first_sem, load_sem, pass_send, pass_recv, cross_send, cross_recv,
    up_send, up_recv, down_send, down_recv, w_send, w_recv,
):
    groups = chans // 2
    me = lax.axis_index("chan")
    slab = lax.axis_index("slab")
    group, core = me // 2, lax.rem(me, 2)
    local_chans, rows, all_cols = beam_ref.shape
    width = all_cols // chans
    chunks = width // LANES
    edge = chunks - 1
    own = groups - 1
    partner = group * 2 + (1 - core)
    not_first, not_last = slab > 0, slab < slabs - 1

    def block_of(slot):
        owner_group = lax.rem(group + slot // 2 + 1, groups)
        return owner_group * 2 + (1 - core if slot % 2 == 0 else core)

    def load(slot, tile):
        col = pl.multiple_of((block_of(slot) * chunks + tile) * LANES, LANES)
        sem = first_sem.at[slot, tile] if isinstance(tile, int) else load_sem.at[tile - FIRST]
        return pltpu.make_async_copy(
            beam_ref.at[:, :, pl.ds(col, LANES)], beams.at[tile, slot], sem
        )

    def drain(ref, sem):
        pltpu.make_async_copy(ref, ref, sem).wait()

    barrier = pltpu.get_barrier_semaphore()
    for offset in range(1, chans):
        pl.semaphore_signal(
            barrier, inc=1, device_id={"chan": lax.rem(me + offset, chans)}, device_id_type=MESH
        )

    @pl.when(not_first)
    def _():
        pl.semaphore_signal(barrier, inc=1, device_id={"slab": slab - 1}, device_id_type=MESH)

    @pl.when(not_last)
    def _():
        pl.semaphore_signal(barrier, inc=1, device_id={"slab": slab + 1}, device_id_type=MESH)

    small = [
        pltpu.make_async_copy(source, target, small_sem.at[at])
        for at, (source, target) in enumerate(((h_hbm, h_ref), (w_hbm, w_ref), (f_hbm, f_ref)))
    ]
    for copy in small:
        copy.start()
    for slots in (range(2 * own), range(2 * own, chans)):
        for tiles in (range(2), range(2, FIRST)):
            for slot in slots:
                for tile in tiles:
                    load(slot, tile).start()

    @pl.loop(FIRST, chunks)
    def _(tile):
        for slot in range(chans):
            load(slot, tile).start()

    source = lax.broadcasted_iota(jnp.int32, (2 * LANES, LANES), 0)
    lane = lax.broadcasted_iota(jnp.int32, (2 * LANES, LANES), 1)
    for copy in small:
        copy.wait()

    def put_band(kind, k, near):
        band[kind, k] = jnp.where(near, 1.0, 0.0).astype(jnp.bfloat16)

    target = jnp.where(lane < HALF, lane + LANES, lane)

    @pl.loop(0, MOMENTS)
    def _(k):
        put_band(0, k, jnp.abs(source - target) <= h_ref[k])

    def weight_copy(offset):
        return pltpu.make_async_remote_copy(
            src_ref=weights.at[0], dst_ref=weights.at[offset],
            send_sem=w_send.at[0], recv_sem=w_recv.at[offset - 1],
            device_id={"chan": lax.rem(me + offset, chans)}, device_id_type=MESH,
        )

    def pass_copy(hop, c):
        return pltpu.make_async_remote_copy(
            src_ref=sums.at[2 * hop, c], dst_ref=passed.at[hop, c],
            send_sem=pass_send.at[hop], recv_sem=pass_recv.at[hop, c],
            device_id={"chan": partner}, device_id_type=MESH,
        )

    def other(hop):
        return lax.rem(group + hop + 1, groups) * 2 + core

    def cross_copy(hop, c, k, half):
        part = pl.ds(half * rows // HALVES, rows // HALVES)
        return pltpu.make_async_remote_copy(
            src_ref=sums.at[2 * hop + 1, c, k, part], dst_ref=crossed.at[hop, c, k, part],
            send_sem=cross_send.at[hop], recv_sem=cross_recv.at[hop, c, k, half],
            device_id={"chan": other(hop)}, device_id_type=MESH,
        )

    def late_copy(hop, j):
        return pltpu.make_async_remote_copy(
            src_ref=late.at[hop, j], dst_ref=crossed.at[hop, 0, MOMENTS - LATE + j],
            send_sem=cross_send.at[hop], recv_sem=cross_recv.at[hop, 0, MOMENTS - LATE + j, 0],
            device_id={"chan": other(hop)}, device_id_type=MESH,
        )

    def place(c, k):
        return c * MOMENTS + k

    def late_place(hop, j):
        if hop == own:
            return place(0, MOMENTS - LATE + j)
        return chunks * MOMENTS + hop * LATE + j

    def up_copy(at):
        return pltpu.make_async_remote_copy(
            src_ref=ext.at[at, pl.ds(HW_MAX, HW_MAX)],
            dst_ref=ext.at[at, pl.ds(HW_MAX + rows, HW_MAX)],
            send_sem=up_send.at[0], recv_sem=up_recv.at[at],
            device_id={"slab": slab - 1}, device_id_type=MESH,
        )

    def down_copy(at):
        return pltpu.make_async_remote_copy(
            src_ref=ext.at[at, pl.ds(rows, HW_MAX)],
            dst_ref=ext.at[at, pl.ds(0, HW_MAX)],
            send_sem=down_send.at[0], recv_sem=down_recv.at[at],
            device_id={"slab": slab + 1}, device_id_type=MESH,
        )

    def moments_of(slot, tile):
        cols = pl.ds(pl.multiple_of((block_of(slot) * chunks + tile + 1) * LANES, LANES), LANES)

        for first in range(0, rows, ROWS_AT_ONCE):
            totals = [None] * MOMENTS
            for chan in range(local_chans):
                weight = w_ref[chan].astype(jnp.float32)
                offset = f_ref[chan]
                term = beams[tile, slot, chan, pl.ds(first, ROWS_AT_ONCE), :] * weight
                for k in range(MOMENTS):
                    if k > 0:
                        term = term * offset
                    totals[k] = term if chan == 0 else totals[k] + term
            for k in range(MOMENTS):
                for at, piece in enumerate(split(totals[k])):
                    pieces[k, pl.ds(first + at * rows, ROWS_AT_ONCE), cols] = piece

    def fold(product):
        result = product[:rows]
        for at in range(1, PARTS):
            result = result + product[at * rows : (at + 1) * rows]
        return result

    def lanes_from(slot, tile):
        first = (block_of(slot) * chunks + tile + 1) * LANES
        return pl.ds(pl.multiple_of(first, LANES), 2 * LANES)

    def columns_of(slot, c):
        wide = lanes_from(slot, c)
        for k in range(MOMENTS):
            sums[slot, c, k] = fold(
                jnp.dot(pieces[k, :, wide], band[0, k], preferred_element_type=jnp.float32)
            )

    def edge_of(slot):
        low, high = lanes_from(slot, -1), lanes_from(slot, chunks - 1)
        for k in range(MOMENTS):
            sums[slot, edge, k] = fold(
                jnp.dot(pieces[k, :, low], band[1, k], preferred_element_type=jnp.float32)
                + jnp.dot(pieces[k, :, high], band[2, k], preferred_element_type=jnp.float32)
            )

    def make(slot, c, following=()):
        if isinstance(c, int) and c == edge:
            edge_of(slot)
        else:
            columns_of(slot, c)
        for other_slot, tile in following:
            moments_of(other_slot, tile)
        if slot % 2 == 0:
            pass_copy(slot // 2, c).start()

    def makes(c):
        jobs = []
        for slot in range(chans):
            if isinstance(c, int) and c == edge:
                following = ()
            elif slot < chans - 1:
                following = ((slot + 1, c + 1),)
            elif isinstance(c, int) and c == edge - 1:
                following = ()
            else:
                following = ((0, c + 2),)
            jobs.append(functools.partial(make, slot, c, following))
        return jobs

    def crosses(c, k):
        return not (isinstance(c, int) and c == 0 and k >= MOMENTS - LATE)

    def send_on(hop, c):
        pass_copy(hop, c).wait_recv()
        for k in range(MOMENTS):
            value = sums[2 * hop + 1, c, k] + passed[hop, c, k]
            if crosses(c, k):
                sums[2 * hop + 1, c, k] = value
                for half in range(HALVES):
                    cross_copy(hop, c, k, half).start()
            else:
                share(late_place(hop, k - MOMENTS + LATE), value)

    def send_up(at):
        @pl.when(not_first)
        def _():
            up_copy(at).start()

    def send_down(at):
        @pl.when(not_last)
        def _():
            down_copy(at).start()

    def share(at, value):
        ext[at, HW_MAX : HW_MAX + rows, :] = value
        send_up(at)
        send_down(at)

    def finish(c, k):
        at = place(c, k)
        for half in range(HALVES):
            first, count = half * rows // HALVES, rows // HALVES
            part = slice(first, first + count)
            value = sums[chans - 1, c, k, part] + passed[own, c, k, part]
            for hop in range(own):
                cross_copy(hop, c, k, half).wait_recv()
                value = value + crossed[hop, c, k, part]
            ext[at, HW_MAX + first : HW_MAX + first + count, :] = value
            if half == 0 and HALVES == 2:
                send_up(at)
        if HALVES == 1:
            send_up(at)
        send_down(at)

    left = lax.broadcasted_iota(jnp.int32, (rows, LANES), 1) < HALF

    def row_sums(at, k):
        @pl.when(not_last)
        def _():
            up_copy(at).wait_recv()

        @pl.when(not_first)
        def _():
            down_copy(at).wait_recv()

        both = jnp.concatenate(split(ext[at]), axis=0)
        return jnp.dot(row_band[k], both, preferred_element_type=jnp.float32)

    def rows_of(c, k):
        if not crosses(c, k):
            return
        summed = row_sums(place(c, k), k) * scale[k, 0:1, :]
        if isinstance(c, int) and c == edge:
            at, to = slice(0, LANES), slice(edge * LANES, chunks * LANES)
            out_ref[k, :, at] = jnp.where(left, summed, out_ref[k, :, at])
            out_ref[k, :, to] = jnp.where(left, out_ref[k, :, to], summed)
        else:
            at = pl.ds(pl.multiple_of(c * LANES, LANES), LANES)
            to = pl.ds(pl.multiple_of((c + 1) * LANES, LANES), LANES)
            if isinstance(c, int) and c == 0:
                out_ref[k, :, at] = summed
            else:
                out_ref[k, :, at] = jnp.where(left, out_ref[k, :, at], summed)
            out_ref[k, :, to] = summed

    def late_rows(hop):
        for j in range(LATE):
            late[hop, j] = row_sums(late_place(hop, j), MOMENTS - LATE + j)

    def late_out(j):
        k = MOMENTS - LATE + j
        summed = late[own, j]
        for hop in range(own):
            late_copy(hop, j).wait_recv()
            summed = summed + crossed[hop, 0, k]
        summed = summed * scale[k, 0:1, :]
        out_ref[k, :, 0:LANES] = jnp.where(left, out_ref[k, :, 0:LANES], summed)
        out_ref[k, :, LANES : 2 * LANES] = jnp.where(
            left, summed, out_ref[k, :, LANES : 2 * LANES]
        )

    @pl.when(slab == 0)
    def _():
        @pl.loop(0, ext.shape[0])
        def _(at):
            ext[at, 0:HW_MAX, :] = jnp.zeros((HW_MAX, LANES), jnp.float32)

    @pl.when(slab == slabs - 1)
    def _():
        @pl.loop(0, ext.shape[0])
        def _(at):
            ext[at, HW_MAX + rows :, :] = jnp.zeros((HW_MAX, LANES), jnp.float32)

    def fetch(tile):
        if not (isinstance(tile, int) and tile >= chunks):
            drain(beams.at[tile], load_sem.at[tile - FIRST])

    def now(*tiles):
        for slot, tile in tiles:
            load(slot, tile).wait()
        return tiles

    for tile in range(2):
        moments_of(*now((0, tile))[0])
    columns_of(0, 0)
    pl.semaphore_wait(
        barrier, chans - 1 + not_first.astype(jnp.int32) + not_last.astype(jnp.int32)
    )
    pass_copy(0, 0).start()
    total = w_ref[0].astype(jnp.float32)
    for chan in range(1, local_chans):
        total = total + w_ref[chan].astype(jnp.float32)
    weights[0] = jnp.full(weights.shape[1:], total, jnp.float32)
    for offset in range(1, chans):
        weight_copy(offset).start()

    for slot in range(1, 2 * own):
        for tile in range(2):
            moments_of(*now((slot, tile))[0])
        make(slot, 0, now((slot - 1, 2)))
        if slot % 2 == 1:
            send_on(slot // 2, 0)
    for slot in range(2 * own - 1):
        make(slot, 1, now((slot + 1, 2)) if slot == 2 * own - 2 else ())
    make(2 * own - 1, 1, now((2 * own, 0)))
    moments_of(*now((2 * own, 1))[0])
    make(2 * own, 0, now((chans - 1, 0), (chans - 1, 1)))
    for hop in range(own):
        send_on(hop, 1)
    make(chans - 1, 0, now((2 * own, 2)))
    make(2 * own, 1, now((chans - 1, 2)))
    fetch(3)
    make(chans - 1, 1, ((0, 3),))
    pass_copy(own, 0).wait_recv()
    for j in range(LATE):
        k = MOMENTS - LATE + j
        share(late_place(own, j), sums[chans - 1, 0, k] + passed[own, 0, k])

    def set_rest():
        out_ref[MOMENTS - LATE :, :, 0 : 2 * LANES] = jnp.zeros(
            (LATE, rows, 2 * LANES), jnp.float32
        )
        pieces[:, :, 0:LANES] = jnp.zeros(pieces.shape[:2] + (LANES,), jnp.bfloat16)
        pieces[:, :, LANES + all_cols :] = jnp.zeros(pieces.shape[:2] + (LANES,), jnp.bfloat16)
        for offset in range(1, chans):
            weight_copy(offset).wait_recv()
        weight_total = weights[0]
        for offset in range(1, chans):
            weight_total = weight_total + weights[offset]

        @pl.loop(0, MOMENTS)
        def _(k):
            reach = h_ref[k]
            near = jnp.logical_and(lane < HALF, jnp.abs(source - LANES - lane) <= reach)
            put_band(1, k, near)
            near = jnp.logical_and(lane >= HALF, jnp.abs(source - lane) <= reach)
            put_band(2, k, near)
            span = rows + 2 * HW_MAX
            to_row = lax.broadcasted_iota(jnp.int32, (rows, span), 0)
            from_row = lax.broadcasted_iota(jnp.int32, (rows, span), 1)
            near = jnp.abs(from_row - HW_MAX - to_row) <= reach
            near = jnp.where(near, 1.0, 0.0).astype(jnp.bfloat16)
            for part in range(PARTS):
                row_band[k, :, part * span : (part + 1) * span] = near
            divisor = weight_total * (2 * reach + 1).astype(jnp.float32)
            scale[k] = 1.0 / divisor

    def iteration(c, ahead, behind):
        jobs = []
        if ahead is not None:
            jobs = makes(ahead)
            fetch(ahead + 2)
        for k in range(MOMENTS):
            if crosses(c, k):
                finish(c, k)
            if k < MOMENTS - 1:
                share = -(-len(jobs) // (MOMENTS - 1 - k))
                for job in jobs[:share]:
                    job()
                jobs = jobs[share:]
            elif ahead is not None:
                for hop in range(own):
                    send_on(hop, ahead)
            if isinstance(c, int) and c == edge and k == LATE_AT:
                for hop in range(own):
                    for j in range(LATE):
                        late_copy(hop, j).start()
            if behind is not None:
                rows_of(behind, k)
        if not (isinstance(c, int) and c == edge):
            pass_copy(own, c + 1).wait_recv()

    iteration(0, 2, None)
    set_rest()
    iteration(1, 3, None)
    for hop in range(groups):
        late_rows(hop)
    iteration(2, 4, 0)

    @pl.loop(3, edge - 3)
    def _(c):
        iteration(c, c + 2, c - 2)

    iteration(edge - 3, edge - 1, edge - 5)
    iteration(edge - 2, edge, edge - 4)
    iteration(edge - 1, None, edge - 3)
    iteration(edge, None, edge - 2)
    for k in range(MOMENTS):
        rows_of(edge - 1, k)
    drain(weights.at[1:chans], w_send.at[0])
    for hop in range(groups):
        drain(sums.at[2 * hop], pass_send.at[hop])
    for k in range(MOMENTS - TAIL):
        rows_of(edge, k)
    for j in range(LATE):
        late_out(j)
    for k in range(MOMENTS - TAIL, MOMENTS):
        rows_of(edge, k)
    for hop in range(own):
        drain(sums.at[2 * hop + 1], cross_send.at[hop])

    @pl.when(not_first)
    def _():
        drain(ext.at[:, HW_MAX : 2 * HW_MAX], up_send.at[0])

    @pl.when(not_last)
    def _():
        drain(ext.at[:, rows : rows + HW_MAX], down_send.at[0])


def body(chans, slabs, beam_images, chan_weights, freq_offsets, half_widths):
    local_chans, rows, all_cols = beam_images.shape
    width = all_cols // chans
    chunks, groups = width // LANES, chans // 2
    f32, b16 = jnp.float32, jnp.bfloat16
    hbm = pl.BlockSpec(memory_space=pltpu.HBM)
    small = [
        pltpu.with_memory_space_constraint(value, pltpu.HBM)
        for value in (chan_weights, freq_offsets, half_widths)
    ]
    span = rows + 2 * HW_MAX
    return pl.pallas_call(
        functools.partial(kernel, chans, slabs),
        out_shape=jax.ShapeDtypeStruct((MOMENTS, rows, width), f32),
        in_specs=[hbm, hbm, hbm, hbm],
        out_specs=pl.BlockSpec(memory_space=pltpu.VMEM),
        scratch_shapes=[
            pltpu.SMEM(chan_weights.shape, jnp.int32),
            pltpu.SMEM(freq_offsets.shape, f32),
            pltpu.SMEM(half_widths.shape, jnp.int32),
            pltpu.VMEM((chunks, chans, local_chans, rows, LANES), f32),
            pltpu.VMEM((MOMENTS, PARTS * rows, all_cols + 2 * LANES), b16),
            pltpu.VMEM((3, MOMENTS, 2 * LANES, LANES), b16),
            pltpu.VMEM((MOMENTS, rows, PARTS * span), b16),
            pltpu.VMEM((chans, chunks, MOMENTS, rows, LANES), f32),
            pltpu.VMEM((groups, chunks, MOMENTS, rows, LANES), f32),
            pltpu.VMEM((groups - 1, chunks, MOMENTS, rows, LANES), f32),
            pltpu.VMEM((chunks * MOMENTS + (groups - 1) * LATE, span, LANES), f32),
            pltpu.VMEM((groups, LATE, rows, LANES), f32),
            pltpu.VMEM((chans, 8, LANES), f32),
            pltpu.VMEM((MOMENTS, 8, LANES), f32),
        ],
        compiler_params=pltpu.CompilerParams(
            collective_id=0, has_side_effects=True, vmem_limit_bytes=44 * 1024 * 1024
        ),
    )(*small, beam_images)


def solution(mesh):
    placed = (P("chan", "slab", None), P("chan"), P("chan"), P())
    return jax.shard_map(
        functools.partial(body, mesh.shape["chan"], mesh.shape["slab"]),
        mesh=mesh, in_specs=placed, out_specs=P(None, "slab", "chan"), check_vma=False,
    )
```

```python
import functools

import jax
import jax.numpy as jnp
from jax import lax
from jax.experimental import pallas as pl
from jax.experimental.pallas import tpu as pltpu
from jax.sharding import PartitionSpec as P

MOMENTS = 5
HW_MAX = 32
LANES = 128
HALF = LANES // 2
PARTS = 2
ROWS_AT_ONCE = 32
FIRST = 3
LATE = 3
LATE_AT = 2
TAIL = 1
HALVES = 2
MESH = pl.DeviceIdType.MESH


def split(value):
    parts = []
    for _ in range(PARTS - 1):
        part = value.astype(jnp.bfloat16)
        parts.append(part)
        value = value - part.astype(jnp.float32)
    parts.append(value.astype(jnp.bfloat16))
    return parts


def kernel(chans, slabs, *refs):
    chunks = refs[3].shape[2] // chans // LANES
    groups = chans // 2
    dma = pltpu.SemaphoreType.DMA
    pl.run_scoped(
        functools.partial(scoped, chans, slabs, *refs),
        dma((3,)),
        dma((chans, FIRST)),
        dma((chunks - FIRST,)),
        dma((groups,)),
        dma((groups, chunks)),
        dma((groups - 1,)),
        dma((groups - 1, chunks, MOMENTS, HALVES)),
        dma((1,)),
        dma((chunks * MOMENTS + (groups - 1) * LATE,)),
        dma((1,)),
        dma((chunks * MOMENTS + (groups - 1) * LATE,)),
        dma((1,)),
        dma((chans - 1,)),
    )


def scoped(
    chans, slabs,
    w_hbm, f_hbm, h_hbm, beam_ref, out_ref,
    w_ref, f_ref, h_ref,
    beams, pieces, band, row_band, sums, passed, crossed, ext, late, weights, scale,
    small_sem, first_sem, load_sem, pass_send, pass_recv, cross_send, cross_recv,
    up_send, up_recv, down_send, down_recv, w_send, w_recv,
):
    groups = chans // 2
    me = lax.axis_index("chan")
    slab = lax.axis_index("slab")
    group, core = me // 2, lax.rem(me, 2)
    local_chans, rows, all_cols = beam_ref.shape
    width = all_cols // chans
    chunks = width // LANES
    edge = chunks - 1
    own = groups - 1
    partner = group * 2 + (1 - core)
    not_first, not_last = slab > 0, slab < slabs - 1

    def block_of(slot):
        owner_group = lax.rem(group + slot // 2 + 1, groups)
        return owner_group * 2 + (1 - core if slot % 2 == 0 else core)

    def load(slot, tile):
        col = pl.multiple_of((block_of(slot) * chunks + tile) * LANES, LANES)
        sem = first_sem.at[slot, tile] if isinstance(tile, int) else load_sem.at[tile - FIRST]
        return pltpu.make_async_copy(
            beam_ref.at[:, :, pl.ds(col, LANES)], beams.at[tile, slot], sem
        )

    def drain(ref, sem):
        pltpu.make_async_copy(ref, ref, sem).wait()

    barrier = pltpu.get_barrier_semaphore()
    for offset in range(1, chans):
        pl.semaphore_signal(
            barrier, inc=1, device_id={"chan": lax.rem(me + offset, chans)}, device_id_type=MESH
        )

    @pl.when(not_first)
    def _():
        pl.semaphore_signal(barrier, inc=1, device_id={"slab": slab - 1}, device_id_type=MESH)

    @pl.when(not_last)
    def _():
        pl.semaphore_signal(barrier, inc=1, device_id={"slab": slab + 1}, device_id_type=MESH)

    small = [
        pltpu.make_async_copy(source, target, small_sem.at[at])
        for at, (source, target) in enumerate(((h_hbm, h_ref), (w_hbm, w_ref), (f_hbm, f_ref)))
    ]
    for copy in small:
        copy.start()
    for slots in (range(2 * own), range(2 * own, chans)):
        for tiles in (range(2), range(2, FIRST)):
            for slot in slots:
                for tile in tiles:
                    load(slot, tile).start()

    @pl.loop(FIRST, chunks)
    def _(tile):
        for slot in range(chans):
            load(slot, tile).start()

    source = lax.broadcasted_iota(jnp.int32, (2 * LANES, LANES), 0)
    lane = lax.broadcasted_iota(jnp.int32, (2 * LANES, LANES), 1)
    for copy in small:
        copy.wait()

    def put_band(kind, k, near):
        band[kind, k] = jnp.where(near, 1.0, 0.0).astype(jnp.bfloat16)

    target = jnp.where(lane < HALF, lane + LANES, lane)

    @pl.loop(0, MOMENTS)
    def _(k):
        put_band(0, k, jnp.abs(source - target) <= h_ref[k])

    def weight_copy(offset):
        return pltpu.make_async_remote_copy(
            src_ref=weights.at[0], dst_ref=weights.at[offset],
            send_sem=w_send.at[0], recv_sem=w_recv.at[offset - 1],
            device_id={"chan": lax.rem(me + offset, chans)}, device_id_type=MESH,
        )

    def pass_copy(hop, c):
        return pltpu.make_async_remote_copy(
            src_ref=sums.at[2 * hop, c], dst_ref=passed.at[hop, c],
            send_sem=pass_send.at[hop], recv_sem=pass_recv.at[hop, c],
            device_id={"chan": partner}, device_id_type=MESH,
        )

    def other(hop):
        return lax.rem(group + hop + 1, groups) * 2 + core

    def cross_copy(hop, c, k, half):
        part = pl.ds(half * rows // HALVES, rows // HALVES)
        return pltpu.make_async_remote_copy(
            src_ref=sums.at[2 * hop + 1, c, k, part], dst_ref=crossed.at[hop, c, k, part],
            send_sem=cross_send.at[hop], recv_sem=cross_recv.at[hop, c, k, half],
            device_id={"chan": other(hop)}, device_id_type=MESH,
        )

    def late_copy(hop, j):
        return pltpu.make_async_remote_copy(
            src_ref=late.at[hop, j], dst_ref=crossed.at[hop, 0, MOMENTS - LATE + j],
            send_sem=cross_send.at[hop], recv_sem=cross_recv.at[hop, 0, MOMENTS - LATE + j, 0],
            device_id={"chan": other(hop)}, device_id_type=MESH,
        )

    def place(c, k):
        return c * MOMENTS + k

    def late_place(hop, j):
        if hop == own:
            return place(0, MOMENTS - LATE + j)
        return chunks * MOMENTS + hop * LATE + j

    def up_copy(at):
        return pltpu.make_async_remote_copy(
            src_ref=ext.at[at, pl.ds(HW_MAX, HW_MAX)],
            dst_ref=ext.at[at, pl.ds(HW_MAX + rows, HW_MAX)],
            send_sem=up_send.at[0], recv_sem=up_recv.at[at],
            device_id={"slab": slab - 1}, device_id_type=MESH,
        )

    def down_copy(at):
        return pltpu.make_async_remote_copy(
            src_ref=ext.at[at, pl.ds(rows, HW_MAX)],
            dst_ref=ext.at[at, pl.ds(0, HW_MAX)],
            send_sem=down_send.at[0], recv_sem=down_recv.at[at],
            device_id={"slab": slab + 1}, device_id_type=MESH,
        )

    def moments_of(slot, tile):
        cols = pl.ds(pl.multiple_of((block_of(slot) * chunks + tile + 1) * LANES, LANES), LANES)

        for first in range(0, rows, ROWS_AT_ONCE):
            totals = [None] * MOMENTS
            for chan in range(local_chans):
                weight = w_ref[chan].astype(jnp.float32)
                offset = f_ref[chan]
                term = beams[tile, slot, chan, pl.ds(first, ROWS_AT_ONCE), :] * weight
                for k in range(MOMENTS):
                    if k > 0:
                        term = term * offset
                    totals[k] = term if chan == 0 else totals[k] + term
            for k in range(MOMENTS):
                for at, piece in enumerate(split(totals[k])):
                    pieces[k, pl.ds(first + at * rows, ROWS_AT_ONCE), cols] = piece

    def fold(product):
        result = product[:rows]
        for at in range(1, PARTS):
            result = result + product[at * rows : (at + 1) * rows]
        return result

    def lanes_from(slot, tile):
        first = (block_of(slot) * chunks + tile + 1) * LANES
        return pl.ds(pl.multiple_of(first, LANES), 2 * LANES)

    def columns_of(slot, c):
        wide = lanes_from(slot, c)
        for k in range(MOMENTS):
            sums[slot, c, k] = fold(
                jnp.dot(pieces[k, :, wide], band[0, k], preferred_element_type=jnp.float32)
            )

    def edge_of(slot):
        low, high = lanes_from(slot, -1), lanes_from(slot, chunks - 1)
        for k in range(MOMENTS):
            sums[slot, edge, k] = fold(
                jnp.dot(pieces[k, :, low], band[1, k], preferred_element_type=jnp.float32)
                + jnp.dot(pieces[k, :, high], band[2, k], preferred_element_type=jnp.float32)
            )

    def make(slot, c, following=()):
        if isinstance(c, int) and c == edge:
            edge_of(slot)
        else:
            columns_of(slot, c)
        for other_slot, tile in following:
            moments_of(other_slot, tile)
        if slot % 2 == 0:
            pass_copy(slot // 2, c).start()

    def makes(c):
        jobs = []
        for slot in range(chans):
            if isinstance(c, int) and c == edge:
                following = ()
            elif slot < chans - 1:
                following = ((slot + 1, c + 1),)
            elif isinstance(c, int) and c == edge - 1:
                following = ()
            else:
                following = ((0, c + 2),)
            jobs.append(functools.partial(make, slot, c, following))
        return jobs

    def crosses(c, k):
        return not (isinstance(c, int) and c == 0 and k >= MOMENTS - LATE)

    def send_on(hop, c):
        pass_copy(hop, c).wait_recv()
        for k in range(MOMENTS):
            value = sums[2 * hop + 1, c, k] + passed[hop, c, k]
            if crosses(c, k):
                sums[2 * hop + 1, c, k] = value
                for half in range(HALVES):
                    cross_copy(hop, c, k, half).start()
            else:
                share(late_place(hop, k - MOMENTS + LATE), value)

    def send_up(at):
        @pl.when(not_first)
        def _():
            up_copy(at).start()

    def send_down(at):
        @pl.when(not_last)
        def _():
            down_copy(at).start()

    def share(at, value):
        ext[at, HW_MAX : HW_MAX + rows, :] = value
        send_up(at)
        send_down(at)

    def finish(c, k):
        at = place(c, k)
        for half in range(HALVES):
            first, count = half * rows // HALVES, rows // HALVES
            part = slice(first, first + count)
            value = sums[chans - 1, c, k, part] + passed[own, c, k, part]
            for hop in range(own):
                cross_copy(hop, c, k, half).wait_recv()
                value = value + crossed[hop, c, k, part]
            ext[at, HW_MAX + first : HW_MAX + first + count, :] = value
            if half == 0 and HALVES == 2:
                send_up(at)
        if HALVES == 1:
            send_up(at)
        send_down(at)

    left = lax.broadcasted_iota(jnp.int32, (rows, LANES), 1) < HALF

    def row_sums(at, k):
        @pl.when(not_last)
        def _():
            up_copy(at).wait_recv()

        @pl.when(not_first)
        def _():
            down_copy(at).wait_recv()

        both = jnp.concatenate(split(ext[at]), axis=0)
        return jnp.dot(row_band[k], both, preferred_element_type=jnp.float32)

    def rows_of(c, k):
        if not crosses(c, k):
            return
        summed = row_sums(place(c, k), k) * scale[k, 0:1, :]
        if isinstance(c, int) and c == edge:
            at, to = slice(0, LANES), slice(edge * LANES, chunks * LANES)
            out_ref[k, :, at] = jnp.where(left, summed, out_ref[k, :, at])
            out_ref[k, :, to] = jnp.where(left, out_ref[k, :, to], summed)
        else:
            at = pl.ds(pl.multiple_of(c * LANES, LANES), LANES)
            to = pl.ds(pl.multiple_of((c + 1) * LANES, LANES), LANES)
            if isinstance(c, int) and c == 0:
                out_ref[k, :, at] = summed
            else:
                out_ref[k, :, at] = jnp.where(left, out_ref[k, :, at], summed)
            out_ref[k, :, to] = summed

    def late_rows(hop):
        for j in range(LATE):
            late[hop, j] = row_sums(late_place(hop, j), MOMENTS - LATE + j)

    def late_out(j):
        k = MOMENTS - LATE + j
        summed = late[own, j]
        for hop in range(own):
            late_copy(hop, j).wait_recv()
            summed = summed + crossed[hop, 0, k]
        summed = summed * scale[k, 0:1, :]
        out_ref[k, :, 0:LANES] = jnp.where(left, out_ref[k, :, 0:LANES], summed)
        out_ref[k, :, LANES : 2 * LANES] = jnp.where(
            left, summed, out_ref[k, :, LANES : 2 * LANES]
        )

    @pl.when(slab == 0)
    def _():
        @pl.loop(0, ext.shape[0])
        def _(at):
            ext[at, 0:HW_MAX, :] = jnp.zeros((HW_MAX, LANES), jnp.float32)

    @pl.when(slab == slabs - 1)
    def _():
        @pl.loop(0, ext.shape[0])
        def _(at):
            ext[at, HW_MAX + rows :, :] = jnp.zeros((HW_MAX, LANES), jnp.float32)

    def fetch(tile):
        if not (isinstance(tile, int) and tile >= chunks):
            drain(beams.at[tile], load_sem.at[tile - FIRST])

    def now(*tiles):
        for slot, tile in tiles:
            load(slot, tile).wait()
        return tiles

    for tile in range(2):
        moments_of(*now((0, tile))[0])
    columns_of(0, 0)
    pl.semaphore_wait(
        barrier, chans - 1 + not_first.astype(jnp.int32) + not_last.astype(jnp.int32)
    )
    pass_copy(0, 0).start()
    total = w_ref[0].astype(jnp.float32)
    for chan in range(1, local_chans):
        total = total + w_ref[chan].astype(jnp.float32)
    weights[0] = jnp.full(weights.shape[1:], total, jnp.float32)
    for offset in range(1, chans):
        weight_copy(offset).start()

    for slot in range(1, 2 * own):
        for tile in range(2):
            moments_of(*now((slot, tile))[0])
        make(slot, 0, now((slot - 1, 2)))
        if slot % 2 == 1:
            send_on(slot // 2, 0)
    for slot in range(2 * own - 1):
        make(slot, 1, now((slot + 1, 2)) if slot == 2 * own - 2 else ())
    make(2 * own - 1, 1, now((2 * own, 0)))
    moments_of(*now((2 * own, 1))[0])
    make(2 * own, 0, now((chans - 1, 0)))
    moments_of(*now((chans - 1, 1))[0])
    for hop in range(own):
        send_on(hop, 1)
    make(chans - 1, 0, now((2 * own, 2)))
    make(2 * own, 1, now((chans - 1, 2)))
    fetch(3)
    pass_copy(own, 0).wait_recv()
    for j in range(LATE):
        k = MOMENTS - LATE + j
        share(late_place(own, j), sums[chans - 1, 0, k] + passed[own, 0, k])
    make(chans - 1, 1, ((0, 3),))

    def set_rest():
        out_ref[MOMENTS - LATE :, :, 0 : 2 * LANES] = jnp.zeros(
            (LATE, rows, 2 * LANES), jnp.float32
        )
        pieces[:, :, 0:LANES] = jnp.zeros(pieces.shape[:2] + (LANES,), jnp.bfloat16)
        pieces[:, :, LANES + all_cols :] = jnp.zeros(pieces.shape[:2] + (LANES,), jnp.bfloat16)
        for offset in range(1, chans):
            weight_copy(offset).wait_recv()
        weight_total = weights[0]
        for offset in range(1, chans):
            weight_total = weight_total + weights[offset]

        @pl.loop(0, MOMENTS)
        def _(k):
            reach = h_ref[k]
            near = jnp.logical_and(lane < HALF, jnp.abs(source - LANES - lane) <= reach)
            put_band(1, k, near)
            near = jnp.logical_and(lane >= HALF, jnp.abs(source - lane) <= reach)
            put_band(2, k, near)
            span = rows + 2 * HW_MAX
            to_row = lax.broadcasted_iota(jnp.int32, (rows, span), 0)
            from_row = lax.broadcasted_iota(jnp.int32, (rows, span), 1)
            near = jnp.abs(from_row - HW_MAX - to_row) <= reach
            near = jnp.where(near, 1.0, 0.0).astype(jnp.bfloat16)
            for part in range(PARTS):
                row_band[k, :, part * span : (part + 1) * span] = near
            divisor = weight_total * (2 * reach + 1).astype(jnp.float32)
            scale[k] = 1.0 / divisor

    def iteration(c, ahead, behind):
        jobs = []
        if ahead is not None:
            jobs = makes(ahead)
            fetch(ahead + 2)
        for k in range(MOMENTS):
            if crosses(c, k):
                finish(c, k)
            if k < MOMENTS - 1:
                share = -(-len(jobs) // (MOMENTS - 1 - k))
                for job in jobs[:share]:
                    job()
                jobs = jobs[share:]
            elif ahead is not None:
                for hop in range(own):
                    send_on(hop, ahead)
            if isinstance(c, int) and c == edge and k == LATE_AT:
                for hop in range(own):
                    for j in range(LATE):
                        late_copy(hop, j).start()
            if behind is not None:
                rows_of(behind, k)
        if not (isinstance(c, int) and c == edge):
            pass_copy(own, c + 1).wait_recv()

    iteration(0, 2, None)
    set_rest()
    iteration(1, 3, None)
    for hop in range(groups):
        late_rows(hop)
    iteration(2, 4, 0)

    @pl.loop(3, edge - 3)
    def _(c):
        iteration(c, c + 2, c - 2)

    iteration(edge - 3, edge - 1, edge - 5)
    iteration(edge - 2, edge, edge - 4)
    iteration(edge - 1, None, edge - 3)
    iteration(edge, None, edge - 2)
    for k in range(MOMENTS):
        rows_of(edge - 1, k)
    drain(weights.at[1:chans], w_send.at[0])
    for hop in range(groups):
        drain(sums.at[2 * hop], pass_send.at[hop])
    for k in range(MOMENTS - TAIL):
        rows_of(edge, k)
    for j in range(LATE):
        late_out(j)
    for k in range(MOMENTS - TAIL, MOMENTS):
        rows_of(edge, k)
    for hop in range(own):
        drain(sums.at[2 * hop + 1], cross_send.at[hop])

    @pl.when(not_first)
    def _():
        drain(ext.at[:, HW_MAX : 2 * HW_MAX], up_send.at[0])

    @pl.when(not_last)
    def _():
        drain(ext.at[:, rows : rows + HW_MAX], down_send.at[0])


def body(chans, slabs, beam_images, chan_weights, freq_offsets, half_widths):
    local_chans, rows, all_cols = beam_images.shape
    width = all_cols // chans
    chunks, groups = width // LANES, chans // 2
    f32, b16 = jnp.float32, jnp.bfloat16
    hbm = pl.BlockSpec(memory_space=pltpu.HBM)
    small = [
        pltpu.with_memory_space_constraint(value, pltpu.HBM)
        for value in (chan_weights, freq_offsets, half_widths)
    ]
    span = rows + 2 * HW_MAX
    return pl.pallas_call(
        functools.partial(kernel, chans, slabs),
        out_shape=jax.ShapeDtypeStruct((MOMENTS, rows, width), f32),
        in_specs=[hbm, hbm, hbm, hbm],
        out_specs=pl.BlockSpec(memory_space=pltpu.VMEM),
        scratch_shapes=[
            pltpu.SMEM(chan_weights.shape, jnp.int32),
            pltpu.SMEM(freq_offsets.shape, f32),
            pltpu.SMEM(half_widths.shape, jnp.int32),
            pltpu.VMEM((chunks, chans, local_chans, rows, LANES), f32),
            pltpu.VMEM((MOMENTS, PARTS * rows, all_cols + 2 * LANES), b16),
            pltpu.VMEM((3, MOMENTS, 2 * LANES, LANES), b16),
            pltpu.VMEM((MOMENTS, rows, PARTS * span), b16),
            pltpu.VMEM((chans, chunks, MOMENTS, rows, LANES), f32),
            pltpu.VMEM((groups, chunks, MOMENTS, rows, LANES), f32),
            pltpu.VMEM((groups - 1, chunks, MOMENTS, rows, LANES), f32),
            pltpu.VMEM((chunks * MOMENTS + (groups - 1) * LATE, span, LANES), f32),
            pltpu.VMEM((groups, LATE, rows, LANES), f32),
            pltpu.VMEM((chans, 8, LANES), f32),
            pltpu.VMEM((MOMENTS, 8, LANES), f32),
        ],
        compiler_params=pltpu.CompilerParams(
            collective_id=0, has_side_effects=True, vmem_limit_bytes=44 * 1024 * 1024
        ),
    )(*small, beam_images)


def solution(mesh):
    placed = (P("chan", "slab", None), P("chan"), P("chan"), P())
    return jax.shard_map(
        functools.partial(body, mesh.shape["chan"], mesh.shape["slab"]),
        mesh=mesh, in_specs=placed, out_specs=P(None, "slab", "chan"), check_vma=False,
    )
```
